32 devices in a mesh: rows: 4 (over y, core), cols: 8 (over z, x).
Axes of the slice: x: 2, y: 2, z: 4, core: 2. Of those that a mesh axis runs over, the one named last changes fastest.
Arguments:
- terrain_grid: float32 [4096, 4096], P('rows', 'cols'), may hold values from -360 to 360
Outputs:
- shade: float32 [4096, 4096], P('rows', 'cols')
- first: float32 [2048, 2048], P('rows', 'cols')
- second: float32 [1024, 1024], P('rows', 'cols')
- third: float32 [512, 512], P('rows', 'cols')
The draws below stay inside these ranges and needn't reach their ends.
All inputs are finite; a program needn't handle non-finite values.
Results may differ from the reference program's by a relative error of at most 0.0003.
Values sent between devices are 32-bit elements; how exact they have to be, the bound alone decides.
No kernel may reach another device: no remote copies, remote signals or barrier semaphores. Data moves between devices by JAX's collectives and lax.ppermute only.
A program may use at most 64 MiB of HBM per device.

```python
import math
import jax
import jax.numpy as jnp
from jax import lax

NEIGHBOUR_REACH = 120
NR = 4096
NC = 4096


def draw_terrain_grid(key, part):
    keys = jax.random.split(key, 9)
    row_pos = jnp.arange(NR, dtype=jnp.float32)[:, None]
    col_pos = jnp.arange(NC, dtype=jnp.float32)[None, :]
    terrain = jnp.zeros((NR, NC), jnp.float32)
    cycles_row = jax.random.uniform(keys[0], (6,), jnp.float32, -3.0, 3.0)
    cycles_col = jax.random.uniform(keys[1], (6,), jnp.float32, -3.0, 3.0)
    phases = jax.random.uniform(keys[2], (6,), jnp.float32, 0.0, 2.0 * math.pi)
    heights = jax.random.uniform(keys[3], (6,), jnp.float32, 20.0, 50.0)
    for number in range(6):
        terrain = terrain + heights[number] * jnp.cos(2.0 * math.pi * (cycles_row[number] * row_pos / NR + cycles_col[number] * col_pos / NC) + phases[number])
    lengths = jnp.exp(jax.random.uniform(keys[4], (8,), jnp.float32, math.log(2.0 * NEIGHBOUR_REACH), math.log(8.0 * NEIGHBOUR_REACH)))
    angles = jax.random.uniform(keys[5], (8,), jnp.float32, -math.pi, math.pi)
    shifts = jax.random.uniform(keys[6], (8,), jnp.float32, 0.0, 2.0 * math.pi)
    ridges = jax.random.uniform(keys[7], (8,), jnp.float32, 2.0, 6.0)
    for number in range(8):
        wave = 2.0 * math.pi / lengths[number]
        terrain = terrain + ridges[number] * jnp.cos(wave * (jnp.cos(angles[number]) * row_pos + jnp.sin(angles[number]) * col_pos) + shifts[number])
    noise = jnp.clip(jax.random.normal(keys[8], (NR, NC), jnp.float32), -5.0, 5.0)
    return terrain + noise


def setup_inputs(seed: int = 0) -> dict:
    streams_of = jax.random.split(jax.random.key(seed), 2)
    return {
        "terrain_grid": draw_terrain_grid(jax.random.fold_in(streams_of[1], 71), 0),
    }


zfactor = 2.0
light_east = -0.5
light_south = -0.5
light_up = math.sqrt(0.5)

def window_extreme(field, count, axis, pick):
    result = field
    power = 1
    while power * 2 <= count:
        length = result.shape[axis] - power
        result = pick(lax.slice_in_dim(result, 0, length, axis=axis), lax.slice_in_dim(result, power, power + length, axis=axis))
        power = power * 2
    rest = count - power
    if rest > 0:
        length = result.shape[axis] - rest
        result = pick(lax.slice_in_dim(result, 0, length, axis=axis), lax.slice_in_dim(result, rest, rest + length, axis=axis))
    return result

def horn_shade(bordered_landform):
    north_west = bordered_landform[:-2, :-2]
    north = bordered_landform[:-2, 1:-1]
    north_east = bordered_landform[:-2, 2:]
    west = bordered_landform[1:-1, :-2]
    east = bordered_landform[1:-1, 2:]
    south_west = bordered_landform[2:, :-2]
    south = bordered_landform[2:, 1:-1]
    south_east = bordered_landform[2:, 2:]
    slope_x = zfactor * (north_east + 2.0 * east + south_east - (north_west + 2.0 * west + south_west)) / 8.0
    slope_y = zfactor * (south_west + 2.0 * south + south_east - (north_west + 2.0 * north + north_east)) / 8.0
    lit = (light_up - light_east * slope_x - light_south * slope_y) / jnp.sqrt(1.0 + slope_x * slope_x + slope_y * slope_y)
    return jnp.maximum(lit, 0.0)

def reduce_level(bordered_landform):
    rows_sum = (bordered_landform[0:-3:2] + 3.0 * bordered_landform[1:-2:2] + 3.0 * bordered_landform[2:-1:2] + bordered_landform[3::2]) / 8.0
    return (rows_sum[:, 0:-3:2] + 3.0 * rows_sum[:, 1:-2:2] + 3.0 * rows_sum[:, 2:-1:2] + rows_sum[:, 3::2]) / 8.0

def reference(terrain_grid):
    bordered_landform = jnp.pad(terrain_grid, NEIGHBOUR_REACH, mode='edge')
    block_rows = math.gcd(NR, 512)
    span = 2 * NEIGHBOUR_REACH + 1

    def rows_block(index):
        piece = lax.dynamic_slice_in_dim(bordered_landform, index * block_rows, block_rows + 2 * NEIGHBOUR_REACH, 0)
        highest = window_extreme(window_extreme(piece, span, 1, jnp.maximum), span, 0, jnp.maximum)
        lowest = window_extreme(window_extreme(piece, span, 1, jnp.minimum), span, 0, jnp.minimum)
        return (highest + lowest) * 0.5
    triangular_filtering = lax.map(rows_block, jnp.arange(NR // block_rows, dtype=jnp.int32))
    triangular_filtering = triangular_filtering.reshape(NR, NC)
    neighbourhood_spread = terrain_grid - triangular_filtering
    shade = horn_shade(jnp.pad(neighbourhood_spread, 1, mode='edge'))
    first = reduce_level(jnp.pad(shade, 1, mode='edge'))
    second = reduce_level(jnp.pad(first, 1, mode='edge'))
    third = reduce_level(jnp.pad(second, 1, mode='edge'))
    return (shade, first, second, third)
```

```python
import functools
import math

import jax
import jax.numpy as jnp
from jax import lax
from jax.experimental import pallas as pl
from jax.experimental.pallas import tpu as pltpu
from jax.sharding import PartitionSpec as P

REACH = 120
HALO = 128
BORDER = 8
LANES = 128
BIG = float("inf")
light_up = math.sqrt(0.5)
VMEM = pl.BlockSpec(memory_space=pltpu.VMEM)
SMEM = pl.BlockSpec(memory_space=pltpu.SMEM)
ANY = pl.BlockSpec(memory_space=pl.ANY)


def fill_halo(dst, top, middle, bottom, at_top, at_bottom, cols):
    rows = middle.shape[0]
    width = middle.shape[1]
    dst[pl.ds(HALO, rows), :] = middle[...]

    @pl.when(at_top)
    def _():
        dst[pl.ds(0, HALO), :] = jnp.broadcast_to(middle[0:1, :], (HALO, width))

    @pl.when(jnp.logical_not(at_top))
    def _():
        dst[pl.ds(0, HALO), :] = top[:, cols]

    @pl.when(at_bottom)
    def _():
        dst[pl.ds(HALO + rows, HALO), :] = jnp.broadcast_to(middle[rows - 1 : rows, :], (HALO, width))

    @pl.when(jnp.logical_not(at_bottom))
    def _():
        dst[pl.ds(HALO + rows, HALO), :] = bottom[:, cols]


def down(t, shift, axis):
    return pltpu.roll(t, (-shift) % t.shape[axis], axis)


def eights(src, dst, pick, lanes, rows):
    block = 80

    def step(i, carry):
        start = pl.multiple_of(i * block, 8)
        t = src[pl.ds(start, block + 8), lanes]
        for shift in (1, 2, 4):
            t = pick(t, down(t, shift, 0))
        dst[pl.ds(start, block), lanes] = t[:block]
        return carry

    lax.fori_loop(0, rows // block, step, 0)


def tall_window(src, w8, dst, pick, lanes, rows):
    block = 208

    def step(i, carry):
        start = pl.multiple_of(i * block, 8)
        t = w8[pl.ds(start, block + 232), lanes]
        for shift in (8, 16, 32, 64):
            length = t.shape[0] - shift
            t = pick(t[:length], t[shift:])
        t = pick(t[:block], t[112:])
        dst[pl.ds(start, block), lanes] = pick(t, src[pl.ds(start + 240, block), lanes])
        return carry

    lax.fori_loop(0, rows // block, step, 0)


def tent(in_lanes, out_lanes, in_size, at_left, at_right):
    shape = (in_lanes, out_lanes)
    col = lax.broadcasted_iota(jnp.int32, shape, 0)
    out = lax.broadcasted_iota(jnp.int32, shape, 1)
    out_size = in_size // 2
    col = jnp.where(col >= in_lanes - LANES // 2, col - in_lanes, col)
    out = jnp.where(out >= out_lanes - LANES // 2, out - out_lanes, out) if out_lanes > out_size else out
    low = jnp.where(at_left, 0, -in_lanes)
    out = jnp.maximum(out, low)
    out = jnp.minimum(out, jnp.where(at_right, out_size - 1, 2 * out_lanes))
    last = jnp.where(at_right, in_size - 1, 2 * in_lanes)
    total = jnp.zeros(shape, jnp.float32)
    for tap, weight in enumerate((0.125, 0.375, 0.375, 0.125)):
        place = jnp.minimum(jnp.maximum(2 * out - 1 + tap, low), last)
        total = total + jnp.where(place == col, weight, 0.0)
    return total.astype(jnp.bfloat16)


def early_kernel(flags, x, top, bottom, inner, high, low, ends, c1, c2, c3, xs, w_high, w_low, v_high, v_low):
    rows, width = x.shape
    at_top, at_bottom = flags[0] == 1, flags[1] == 1
    at_left, at_right = flags[2] == 1, flags[3] == 1
    fill_halo(xs, top, x, bottom, at_top, at_bottom, slice(None))
    tall = rows + 2 * BORDER
    for tile in range(width // LANES):
        lanes = pl.ds(tile * LANES, LANES)
        for pick, w8, v in ((jnp.maximum, w_high, v_high), (jnp.minimum, w_low, v_low)):
            eights(xs, w8, pick, lanes, rows + 2 * HALO)
            tall_window(xs, w8, v, pick, lanes, tall)
    block = 208
    last = width - LANES

    def step(i, carry):
        start = pl.multiple_of(i * block, 8)
        wide = []
        for pick, v, spare in ((jnp.maximum, v_high, -BIG), (jnp.minimum, v_low, BIG)):
            t = jnp.concatenate([v[pl.ds(start, block), :], jnp.full((block, LANES), spare, jnp.float32)], axis=1)
            for shift in (1, 2, 4, -8, -16, -32, -64, 113):
                t = pick(t, down(t, shift, 1))
            wide.append(t)
        h, l = wide
        own = xs[pl.ds(start + REACH, block), :]
        inner[pl.ds(start + BORDER, block), :] = own[:, LANES:last] - 0.5 * (h[:, LANES:last] + l[:, LANES:last])
        for out, t in ((high, h), (low, l)):
            out[pl.ds(start, block), pl.ds(0, LANES)] = t[:, :LANES]
            out[pl.ds(start, block), pl.ds(LANES, 2 * LANES)] = t[:, last:]
        ends[pl.ds(start, block), pl.ds(0, LANES)] = own[:, :LANES]
        ends[pl.ds(start, block), pl.ds(LANES, LANES)] = own[:, last:]
        return carry

    lax.fori_loop(0, tall // block, step, 0)
    fix_rows(inner, 2 * BORDER, rows, at_top, at_bottom)
    m1 = tent(width + LANES, width // 2 + LANES, width, at_left, at_right)
    m2 = tent(width // 2 + LANES, width // 4 + LANES, width // 2, at_left, at_right)
    m3 = tent(width // 4 + LANES, LANES, width // 4, at_left, at_right)
    c1[...] = m1[:, : width // 2]
    m12 = jnp.dot(m1, m2, preferred_element_type=jnp.float32).astype(jnp.bfloat16)
    c2[...] = m12[:, : width // 4]
    c3[...] = jnp.dot(m12, m3, preferred_element_type=jnp.float32).astype(jnp.bfloat16)


def fix_rows(ref, first, rows, at_top, at_bottom):
    @pl.when(at_top)
    def _():
        ref[pl.ds(first - 1, 1), :] = ref[pl.ds(first, 1), :]

    @pl.when(at_bottom)
    def _():
        ref[pl.ds(first + rows, 1), :] = ref[pl.ds(first + rows - 1, 1), :]


def two_pass(t, m):
    head = t.astype(jnp.bfloat16)
    tail = (t - head.astype(jnp.float32)).astype(jnp.bfloat16)
    return jnp.dot(head, m, preferred_element_type=jnp.float32) + jnp.dot(tail, m, preferred_element_type=jnp.float32)


def halve_rows(ref, start, count):
    tiles = []
    for tile in range(ref.shape[0]):
        a, b, c, d = (ref[tile, pl.ds(start + tap, count, stride=2), :] for tap in range(4))
        tiles.append(((a + d) + 3.0 * (b + c)) * 0.125)
    return tiles


def put_tiles(ref, count, tiles):
    for tile, t in enumerate(tiles):
        ref[tile, pl.ds(0, count), :] = t


def wide(ref, count):
    return jnp.concatenate([ref[tile, pl.ds(0, count), :] for tile in range(ref.shape[0])], axis=1)


def late_kernel(
    flags, left, right, top, bottom, inner, high, low, ends, c1, c2, c3,
    shade, first, second, third,
    xl, xr, s_high, s_low, p_high, p_low, w8, v_sh, v_sl, v_ph, v_pl, rel, lit, u1, u2, f1, f2, f3, sems,
):
    rows = left.shape[0]
    width = inner.shape[1] + 2 * LANES
    tall = rows + 2 * BORDER
    at_top, at_bottom = flags[0] == 1, flags[1] == 1
    at_left, at_right = flags[2] == 1, flags[3] == 1
    fill_halo(xl, top, left, bottom, at_top, at_bottom, slice(0, LANES))
    fill_halo(xr, top, right, bottom, at_top, at_bottom, slice(LANES, 2 * LANES))
    whole = pl.ds(0, LANES)
    block = 320

    def scan(i, carry):
        start = pl.multiple_of(i * block, 8)
        lane = lax.broadcasted_iota(jnp.int32, (block, LANES), 1)
        for src, gone, sign, out_high, out_low in ((xl, at_left, 1, s_high, s_low), (xr, at_right, -1, p_high, p_low)):
            t = src[pl.ds(start, block), :]
            for pick, spare, out in ((jnp.maximum, -BIG, out_high), (jnp.minimum, BIG, out_low)):
                r = jnp.where(gone, spare, t)
                for shift in (1, 2, 4, 8, 16, 32, 64):
                    inside = lane < LANES - shift if sign > 0 else lane >= shift
                    r = pick(r, jnp.where(inside, down(r, sign * shift, 1), spare))
                out[pl.ds(start, block), :] = down(r, sign * BORDER, 1)
        return carry

    lax.fori_loop(0, (rows + 2 * HALO) // block, scan, 0)
    for src, out, pick in (
        (s_high, v_sh, jnp.maximum),
        (s_low, v_sl, jnp.minimum),
        (p_high, v_ph, jnp.maximum),
        (p_low, v_pl, jnp.minimum),
    ):
        eights(src, w8, pick, whole, rows + 2 * HALO)
        tall_window(src, w8, out, pick, whole, tall)

    block2 = 208

    def combine(i, carry):
        start = pl.multiple_of(i * block2, 8)
        here = pl.ds(start, block2)
        there = pl.ds(start + BORDER, block2)
        lane = lax.broadcasted_iota(jnp.int32, (block2, LANES), 1)
        sh, sl, ph, pw = v_sh[here, :], v_sl[here, :], v_ph[here, :], v_pl[here, :]
        near, far, spare = pl.ds(0, LANES), pl.ds(LANES, LANES), pl.ds(2 * LANES, LANES)
        body = lane < LANES - BORDER
        h = jnp.maximum(high[here, near], jnp.where(body, sh, -BIG))
        l = jnp.minimum(low[here, near], jnp.where(body, sl, BIG))
        rel[there, near] = ends[here, near] - 0.5 * (h + l)
        body = lane >= BORDER
        h = jnp.maximum(high[here, far], jnp.where(body, ph, -BIG))
        l = jnp.minimum(low[here, far], jnp.where(body, pw, BIG))
        rel[there, far] = ends[here, far] - 0.5 * (h + l)
        mine = lane < LANES // 2
        h = jnp.maximum(high[here, spare], jnp.where(mine, ph, sh))
        l = jnp.minimum(low[here, spare], jnp.where(mine, pw, sl))
        strip = pl.ds(start + REACH, block2)
        rel[there, spare] = jnp.where(mine, xr[strip, :], xl[strip, :]) - 0.5 * (h + l)
        return carry

    lax.fori_loop(0, tall // block2, combine, 0)
    fix_rows(rel, 2 * BORDER, rows, at_top, at_bottom)

    def shading(i, carry):
        start = pl.multiple_of(i * block2, 8)
        here = pl.ds(start, block2 + 2 * BORDER)
        p = jnp.concatenate([rel[here, pl.ds(0, LANES)], inner[here, :], rel[here, pl.ds(LANES, 2 * LANES)]], axis=1)
        north, south = down(p, -1, 0), down(p, 1, 0)
        v = (north + south) + 2.0 * p
        d = south - north
        lane = lax.broadcasted_iota(jnp.int32, (block2 + 2 * BORDER, LANES), 1)
        west_edge = jnp.logical_and(lane == 0, at_left)
        east_edge = jnp.logical_and(lane == LANES - 1, at_right)

        def west(t):
            s = down(t, -1, 1)
            return jnp.concatenate([jnp.where(west_edge, t[:, :LANES], s[:, :LANES]), s[:, LANES:]], axis=1)

        def east(t):
            s = down(t, 1, 1)
            a, b = width - LANES, width
            return jnp.concatenate([s[:, :a], jnp.where(east_edge, t[:, a:b], s[:, a:b]), s[:, b:]], axis=1)

        gx = 0.25 * (east(v) - west(v))
        gy = 0.25 * ((east(d) + west(d)) + 2.0 * d)
        lum = (light_up + 0.5 * (gx + gy)) * lax.rsqrt(1.0 + gx * gx + gy * gy)
        lum = jnp.maximum(lum, 0.0)[BORDER : BORDER + block2]
        for tile in range(lit.shape[0]):
            lit[tile, pl.ds(start, block2), :] = lum[:, tile * LANES : (tile + 1) * LANES]
        return carry

    lax.fori_loop(0, tall // block2, shading, 0)
    tiles = width // LANES
    copies = []
    for tile in range(tiles):
        out = shade.at[:, pl.ds(tile * LANES, LANES)]
        copies.append(pltpu.make_async_copy(lit.at[tile, pl.ds(BORDER, rows), :], out, sems.at[tile]))
        copies[-1].start()
    fix_tile_rows(lit, BORDER, rows, at_top, at_bottom)
    n1 = rows // 2 + BORDER
    put_tiles(u1, n1, halve_rows(lit, 1, n1))
    fix_tile_rows(u1, 3, rows // 2, at_top, at_bottom)
    n2 = rows // 4 + BORDER
    put_tiles(u2, n2, halve_rows(u1, 0, n2))
    fix_tile_rows(u2, 1, rows // 4, at_top, at_bottom)
    f1[...] = two_pass(wide(u1, n1), c1[...])[3 : 3 + rows // 2]
    f2[...] = two_pass(wide(u2, n2), c2[...])[1 : 1 + rows // 4]
    f3[...] = two_pass(jnp.concatenate(halve_rows(u2, 0, rows // 8), axis=1), c3[...])[:, : width // 8]
    for number, (src, out) in enumerate(((f1, first), (f2, second), (f3, third))):
        copy = pltpu.make_async_copy(src, out, sems.at[tiles + number])
        copy.start()
        copies.append(copy)
    for copy in copies:
        copy.wait()


def fix_tile_rows(ref, first, rows, at_top, at_bottom):
    for tile in range(ref.shape[0]):
        fix_rows(ref.at[tile], first, rows, at_top, at_bottom)


def on_device(x):
    rows, width = x.shape
    n_rows, n_cols = lax.axis_size("rows"), lax.axis_size("cols")
    my_row, my_col = lax.axis_index("rows"), lax.axis_index("cols")
    flags = jnp.stack([my_row == 0, my_row == n_rows - 1, my_col == 0, my_col == n_cols - 1]).astype(jnp.int32)

    def steps(count):
        up = [(i, i + 1) for i in range(count - 1)]
        return up, [(j, i) for i, j in up]

    right_going, left_going = steps(n_cols)
    south_going, north_going = steps(n_rows)
    left = lax.ppermute(x[:, width - LANES :], "cols", right_going)
    right = lax.ppermute(x[:, :LANES], "cols", left_going)
    top = lax.ppermute(x[rows - HALO :], "rows", south_going)
    bottom = lax.ppermute(x[:HALO], "rows", north_going)
    both = lambda a, b: jnp.concatenate([left[a:b], right[a:b]], axis=1)
    corner_top = lax.ppermute(both(rows - HALO, rows), "rows", south_going)
    corner_bottom = lax.ppermute(both(0, HALO), "rows", north_going)

    f32 = jnp.float32
    tall, deep = rows + 2 * BORDER, rows + 2 * HALO
    shape = jax.ShapeDtypeStruct
    limit = pltpu.CompilerParams(vmem_limit_bytes=48 * 2**20)
    early = pl.pallas_call(
        early_kernel,
        name="early",
        in_specs=[SMEM, VMEM, VMEM, VMEM],
        out_specs=[VMEM] * 7,
        out_shape=[
            shape((tall + 2 * BORDER, width - 2 * LANES), f32),
            shape((tall, 3 * LANES), f32),
            shape((tall, 3 * LANES), f32),
            shape((tall, 2 * LANES), f32),
            shape((width + LANES, width // 2), jnp.bfloat16),
            shape((width + LANES, width // 4), jnp.bfloat16),
            shape((width + LANES, LANES), jnp.bfloat16),
        ],
        scratch_shapes=[pltpu.VMEM((deep + 8, width), f32)] * 3 + [pltpu.VMEM((tall, width), f32)] * 2,
        compiler_params=limit,
        cost_estimate=pl.CostEstimate(flops=80_000_000, bytes_accessed=8_000_000, transcendentals=0),
    )(flags, x, top, bottom)
    strip = pltpu.VMEM((deep + 8, LANES), f32)
    column = pltpu.VMEM((tall, LANES), f32)
    return pl.pallas_call(
        late_kernel,
        name="late",
        in_specs=[SMEM] + [VMEM] * 11,
        out_specs=[ANY] * 4,
        out_shape=[shape((rows >> k, width >> k), f32) for k in range(4)],
        scratch_shapes=[strip] * 7
        + [column] * 4
        + [
            pltpu.VMEM((tall + 2 * BORDER, 3 * LANES), f32),
            pltpu.VMEM((width // LANES + 1, tall + BORDER, LANES), f32),
            pltpu.VMEM((width // LANES + 1, rows // 2 + 3 * BORDER, LANES), f32),
            pltpu.VMEM((width // LANES + 1, rows // 4 + 2 * BORDER, LANES), f32),
            pltpu.VMEM((rows // 2, width // 2), f32),
            pltpu.VMEM((rows // 4, width // 4), f32),
            pltpu.VMEM((rows // 8, width // 8), f32),
            pltpu.SemaphoreType.DMA((width // LANES + 3,)),
        ],
        compiler_params=limit,
        cost_estimate=pl.CostEstimate(flops=80_000_000, bytes_accessed=8_000_000, transcendentals=0),
    )(flags, left, right, corner_top, corner_bottom, *early)


def solution(mesh):
    spec = P("rows", "cols")
    return jax.shard_map(on_device, mesh=mesh, in_specs=(spec,), out_specs=(spec,) * 4, check_vma=False)
```

```python
import math

import jax
import jax.numpy as jnp
from jax import lax
from jax.experimental import pallas as pl
from jax.experimental.pallas import tpu as pltpu
from jax.sharding import PartitionSpec as P

REACH = 120
HALO = 128
BORDER = 8
LANES = 128
BIG = float("inf")
light_up = math.sqrt(0.5)
VMEM = pl.BlockSpec(memory_space=pltpu.VMEM)
ANY = pl.BlockSpec(memory_space=pl.ANY)
HBM = pl.BlockSpec(memory_space=pltpu.HBM)
PICKS = ((jnp.maximum, -BIG), (jnp.minimum, BIG))


class Place:
    def __init__(self):
        row, col = lax.axis_index("rows"), lax.axis_index("cols")
        self.top, self.bottom = row == 0, row == lax.axis_size("rows") - 1
        self.left, self.right = col == 0, col == lax.axis_size("cols") - 1
        self.even_row, self.even_col = row % 2 == 0, col % 2 == 0


def down(t, shift, axis):
    return pltpu.roll(t, (-shift) % t.shape[axis], axis)


def multiple(i, size):
    return pl.multiple_of(i * size, size)


def fours(srcs, dsts, offset, rows, block):
    def step(i, carry):
        start = offset + multiple(i, block)
        both = [[src[pl.ds(start + tap, block), :] for tap in range(4)] for src in srcs]
        for (pick, _), (a, b, c, d), dst in zip(PICKS, both * (2 // len(srcs)), dsts):
            dst[pl.ds(start, block), :] = pick(pick(a, b), pick(c, d))
        return carry

    lax.fori_loop(0, rows // block, step, 0)


def tall_window(src, w4, put, pick, groups, first=0, last=1 << 20):
    levels = [{} for _ in range(5)]

    def join(a, b):
        return a if b is None else b if a is None else pick(a, b)

    def cells(g):
        return src[pl.ds(8 * g, 8), :] if first <= g < last else None

    def eight(g):
        return pick(w4[pl.ds(8 * g, 8), :], w4[pl.ds(8 * g + 4, 8), :]) if first - 1 <= g < last else None

    for g in range(groups + 29):
        levels[0][g] = eight(g)
        at = g
        for level, shift in enumerate((1, 2, 4, 8)):
            at -= shift
            if at >= 0:
                levels[level + 1][at] = join(levels[level].pop(at), levels[level][at + shift])
        out = g - 29
        if out >= 0:
            put(out, join(join(levels[4].pop(out), levels[4][out + 14]), cells(out + 30)))


def tent(in_lanes, out_lanes, in_size, place):
    shape = (in_lanes, out_lanes)
    col = lax.broadcasted_iota(jnp.int32, shape, 0)
    out = lax.broadcasted_iota(jnp.int32, shape, 1)
    out_size = in_size // 2
    col = jnp.where(col >= in_lanes - LANES // 2, col - in_lanes, col)
    out = jnp.where(out >= out_lanes - LANES // 2, out - out_lanes, out) if out_lanes > out_size else out
    low = jnp.where(place.left, 0, -in_lanes)
    out = jnp.maximum(out, low)
    out = jnp.minimum(out, jnp.where(place.right, out_size - 1, 2 * out_lanes))
    last = jnp.where(place.right, in_size - 1, 2 * in_lanes)
    total = jnp.zeros(shape, jnp.float32)
    for tap, weight in enumerate((0.125, 0.375, 0.375, 0.125)):
        spot = jnp.minimum(jnp.maximum(2 * out - 1 + tap, low), last)
        total = total + jnp.where(spot == col, weight, 0.0)
    return total.astype(jnp.bfloat16)


def fix_rows(ref, first, rows, place):
    @pl.when(place.top)
    def _():
        for tile in range(ref.shape[0]):
            ref[tile, pl.ds(first - 1, 1), :] = ref[tile, pl.ds(first, 1), :]

    @pl.when(place.bottom)
    def _():
        for tile in range(ref.shape[0]):
            ref[tile, pl.ds(first + rows, 1), :] = ref[tile, pl.ds(first + rows - 1, 1), :]


def slopes(p, west, east):
    return east - west, (east + west) + (p + p)


def shading(ab, lit, rows, block):
    count = ab.shape[0] // 2

    def step(i, carry):
        start = multiple(i, block)
        for tile in range(count):
            a = ab.at[2 * tile]
            b = ab.at[2 * tile + 1]
            north, here, south = (pl.ds(start + BORDER + shift, block) for shift in (-1, 0, 1))
            mid = a[here, :]
            gx = (a[north, :] + a[south, :]) + (mid + mid)
            gy = b[south, :] - b[north, :]
            lum = (light_up + 0.125 * (gx + gy)) * lax.rsqrt(1.0 + 0.0625 * (gx * gx + gy * gy))
            lit[tile, pl.ds(start, block), :] = jnp.maximum(lum, 0.0)
        return carry

    lax.fori_loop(0, rows // block, step, 0)


def halve_rows(src, dst, start, count):
    for tile in range(src.shape[0]):
        a, b, c, d = (src[tile, pl.ds(start + tap, count, stride=2), :] for tap in range(4))
        dst[tile, pl.ds(0, count), :] = ((a + d) + 3.0 * (b + c)) * 0.125


def row_levels(lit, u1, u2, u3, rows, place):
    fix_rows(lit, BORDER, rows, place)
    halve_rows(lit, u1, 1, rows // 2 + BORDER)
    fix_rows(u1, 3, rows // 2, place)
    halve_rows(u1, u2, 0, rows // 4 + BORDER)
    fix_rows(u2, 1, rows // 4, place)
    halve_rows(u2, u3, 0, rows // 8)


def lane_index(rows):
    return lax.broadcasted_iota(jnp.int32, (rows, LANES), 1)


def pack_kernel(x, a_ends, b_ends, a_mid, b_mid, to_y, to_core, sems):
    place = Place()
    rows, width = x.shape
    far = pl.multiple_of(width - LANES + 0 * lax.axis_index("cols"), LANES)
    a_lanes = pl.ds(pl.multiple_of(jnp.where(place.even_col, far, 0), LANES), LANES)
    b_lanes = pl.ds(pl.multiple_of(jnp.where(place.even_col, 0, far), LANES), LANES)
    low = rows - HALO
    y_rows = pl.ds(pl.multiple_of(jnp.where(place.even_row, 0, low), HALO), HALO)
    core_rows = pl.ds(pl.multiple_of(jnp.where(place.even_row, low, 0), HALO), HALO)
    pairs = []
    for lanes, ends, mid in ((b_lanes, b_ends, b_mid), (a_lanes, a_ends, a_mid)):
        pairs.append((x.at[pl.ds(0, HALO), lanes], ends.at[pl.ds(0, HALO), :]))
        pairs.append((x.at[pl.ds(low, HALO), lanes], ends.at[pl.ds(HALO, HALO), :]))
        pairs.append((x.at[pl.ds(HALO, low - HALO), lanes], mid))
    pairs.append((x.at[y_rows, :], to_y))
    pairs.append((x.at[core_rows, :], to_core))
    copies = [pltpu.make_async_copy(src, dst, sems.at[number]) for number, (src, dst) in enumerate(pairs)]
    for copy in copies:
        copy.start()
    for copy in copies:
        copy.wait()


def corner_kernel(a_ends, b_ends, to_y, to_core):
    even_row = Place().even_row
    y_rows = pl.ds(pl.multiple_of(jnp.where(even_row, 0, HALO), HALO), HALO)
    core_rows = pl.ds(pl.multiple_of(jnp.where(even_row, HALO, 0), HALO), HALO)
    for number, ends in enumerate((a_ends, b_ends)):
        lanes = pl.ds(number * LANES, LANES)
        to_y[:, lanes] = ends[y_rows, :]
        to_core[:, lanes] = ends[core_rows, :]


def halo_rows(dst, rows, by_core, by_y, first, last, place):
    below = HALO + rows

    @pl.when(jnp.logical_and(place.even_row, jnp.logical_not(place.top)))
    def _():
        dst(0, by_y)

    @pl.when(jnp.logical_not(place.even_row))
    def _():
        dst(0, by_core)

    @pl.when(jnp.logical_and(place.even_row, jnp.logical_not(place.bottom)))
    def _():
        dst(below, by_core)

    @pl.when(jnp.logical_and(jnp.logical_not(place.even_row), jnp.logical_not(place.bottom)))
    def _():
        dst(below, by_y)

    @pl.when(place.top)
    def _():
        dst(0, first)

    @pl.when(place.bottom)
    def _():
        dst(below, last)


def early_kernel(
    x, by_core, by_y,
    high, low, ends, beside, lit, u1, u2, u3, c1, c2, c3,
    xs, w_high, w_low, v_high, v_low, t_high, t_low, h_high, h_low, ab,
):
    place = Place()
    rows, width = x.shape
    tiles = width // LANES
    tall, deep = rows + 2 * BORDER, rows + 2 * HALO
    lanes_of = [slice(tile * LANES, (tile + 1) * LANES) for tile in range(tiles)]
    for tile in range(tiles):
        xs[tile, pl.ds(HALO, rows), :] = x[:, lanes_of[tile]]

    def whole_row(start, value):
        for tile in range(tiles):
            xs[tile, pl.ds(start, HALO), :] = jnp.broadcast_to(value[:, lanes_of[tile]], (HALO, LANES))

    halo_rows(whole_row, rows, by_core, by_y, x.at[pl.ds(0, 1), :], x.at[pl.ds(rows - 1, 1), :], place)

    def vertical(tile, carry):
        src = xs.at[tile]
        fours((src,), (w_high, w_low), 0, deep, 80)
        for (pick, _), w4, v in zip(PICKS, (w_high, w_low), (v_high, v_low)):

            def put(g, value, v=v):
                v[tile, pl.ds(8 * g, 8), :] = value

            tall_window(src, w4, put, pick, tall // 8)
        return carry

    lax.fori_loop(0, tiles, vertical, 0)

    for (_, spare), t, w in zip(PICKS, (t_high, t_low), (w_high, w_low)):
        for start in (0, HALO + width):
            t[pl.ds(start, HALO), :] = jnp.full((HALO, LANES), spare, jnp.float32)
        w[pl.ds(HALO + width, HALO), :] = jnp.full((HALO, LANES), spare, jnp.float32)

    def columns(i, carry):
        here = pl.ds(multiple(i, LANES), LANES)
        for v, t in ((v_high, t_high), (v_low, t_low)):
            for tile in range(tiles):
                t[pl.ds(HALO + tile * LANES, LANES), :] = v[tile, here, :].T
        fours((t_high, t_low), (w_high, w_low), REACH, width + BORDER, 104)
        for (pick, _), t, w4, h in zip(PICKS, (t_high, t_low), (w_high, w_low), (h_high, h_low)):

            def put(g, value, h=h):
                h[pl.ds(8 * g, 8), :] = value

            tall_window(t, w4, put, pick, (width + 2 * BORDER) // 8, HALO // 8, (HALO + width) // 8)
        own = pl.ds(multiple(i, LANES) + REACH, LANES)
        there = pl.ds(multiple(i, LANES) + BORDER, LANES)
        p = []
        for tile in range(tiles):
            at = pl.ds(BORDER + tile * LANES, LANES)
            mine = xs[tile, own, :]
            if tile in (0, tiles - 1):
                into = min(tile, 1)
                hi, lo = h_high[at, :].T, h_low[at, :].T
                high[into, here, :] = hi
                low[into, here, :] = lo
                ends[into, here, :] = mine
                p.append(mine - 0.5 * (hi + lo))
            else:
                p.append(mine - 0.5 * (h_high[at, :] + h_low[at, :]).T)
        for h, out in ((h_high, high), (h_low, low)):
            t = [h[pl.ds(width + BORDER, BORDER), :], h[pl.ds(2 * BORDER, LANES - 2 * BORDER), :], h[pl.ds(0, BORDER), :]]
            out[2, here, :] = jnp.concatenate(t, axis=0).T
        lane = lane_index(LANES)
        wests = [down(t, -1, 1) for t in p[:-1]]
        easts = [down(t, 1, 1) for t in p[1:]]
        for tile in range(1, tiles - 1):
            w = jnp.where(lane == 0, wests[tile - 1], wests[tile])
            e = jnp.where(lane == LANES - 1, easts[tile], easts[tile - 1])
            ab[2 * tile - 2, there, :], ab[2 * tile - 1, there, :] = slopes(p[tile], w, e)
        beside[here, :] = jnp.where(lane < LANES // 2, p[1], p[tiles - 2])
        return carry

    lax.fori_loop(0, pl.cdiv(tall, LANES), columns, 0)
    fix_rows(ab, 2 * BORDER, rows, place)
    shading(ab, lit, tall, 104)
    row_levels(lit, u1, u2, u3, rows, place)
    m1 = tent(width + LANES, width // 2 + LANES, width, place)
    m2 = tent(width // 2 + LANES, width // 4 + LANES, width // 2, place)
    m3 = tent(width // 4 + LANES, LANES, width // 4, place)
    c1[...] = m1[:, : width // 2]
    m12 = jnp.dot(m1, m2, preferred_element_type=jnp.float32).astype(jnp.bfloat16)
    c2[...] = m12[:, : width // 4]
    c3[...] = jnp.dot(m12, m3, preferred_element_type=jnp.float32).astype(jnp.bfloat16)


def two_pass(t, m):
    head = t.astype(jnp.bfloat16)
    tail = (t - head.astype(jnp.float32)).astype(jnp.bfloat16)
    return jnp.dot(head, m, preferred_element_type=jnp.float32) + jnp.dot(tail, m, preferred_element_type=jnp.float32)


def running(t, work, w4, pick, spare, sign):
    n = t.shape[0] // 8
    order = range(n - 1, -1, -1) if sign > 0 else range(n)
    total = None
    for g in order:
        part = t[8 * g : 8 * g + 8]
        total = part if total is None else pick(total, part)
        work[pl.ds(8 * g + 8, 8), :] = total
    work[pl.ds(8 * n + 8 if sign > 0 else 0, 8), :] = jnp.full((8, t.shape[1]), spare, jnp.float32)
    rows = 8 * n + 8 - 4
    base = 8 if sign > 0 else 1
    a, b, c, d = (work[pl.ds(base + tap, rows), :] for tap in range(4))
    w4[pl.ds(0, rows), :] = pick(pick(a, b), pick(c, d))
    return pick(w4[pl.ds(0, 8 * n), :], w4[pl.ds(4, 8 * n), :])


def late_kernel(
    a_ends, b_ends, a_mid, b_mid, by_core, by_y, high, low, ends, beside, lit_in, u1_in, u2_in, u3_in, c1, c2, c3,
    shade, first, second, third,
    strips, scans, work, w4s, w_high, w_low, walls, ab, lit, u1, u2, u3, f1, f2, f3, sems,
):
    place = Place()
    rows = a_mid.shape[0] + 2 * HALO
    tiles = lit_in.shape[0] + 2
    width = tiles * LANES
    tall, deep = rows + 2 * BORDER, rows + 2 * HALO
    copies = []

    def send(src, out, number):
        copies.append(pltpu.make_async_copy(src, out, sems.at[number]))
        copies[-1].start()

    def send_tile(src, tile):
        send(src.at[pl.ds(BORDER, rows), :], shade.at[:, pl.ds(tile * LANES, LANES)], tile)

    for tile in range(1, tiles - 1):
        send_tile(lit_in.at[tile - 1], tile)

    for kind, (tips, mid) in enumerate(((a_ends, a_mid), (b_ends, b_mid))):
        dst = strips.at[jnp.where(place.even_col, 1 - kind, kind)]
        lanes = pl.ds(kind * LANES, LANES)
        dst[pl.ds(HALO, HALO), :] = tips[pl.ds(0, HALO), :]
        dst[pl.ds(2 * HALO, rows - 2 * HALO), :] = mid[...]
        dst[pl.ds(rows, HALO), :] = tips[pl.ds(HALO, HALO), :]

        def write(start, value, dst=dst):
            dst[pl.ds(start, HALO), :] = jnp.broadcast_to(value[...], (HALO, LANES))

        edges = (tips.at[pl.ds(0, 1), :], tips.at[pl.ds(2 * HALO - 1, 1), :])
        halo_rows(write, rows, by_core.at[:, lanes], by_y.at[:, lanes], *edges, place)

    def scan(i, carry):
        here = pl.ds(multiple(i, LANES), LANES)
        for side, (sign, gone) in enumerate(((1, place.left), (-1, place.right))):
            t = strips[side, here, :].T
            for number, (pick, spare) in enumerate(PICKS):
                slot = 2 * side + number
                r = running(jnp.where(gone, spare, t), work.at[slot], w4s.at[slot], pick, spare, sign)
                r = jnp.concatenate([r[BORDER:], r[:BORDER]] if sign > 0 else [r[-BORDER:], r[:-BORDER]], axis=0)
                scans[slot, here, :] = r.T
        return carry

    lax.fori_loop(0, deep // LANES, scan, 0)

    def vertical(side, carry):
        srcs = (scans.at[2 * side], scans.at[2 * side + 1])
        fours(srcs, (w_high, w_low), 0, deep, 80)
        for number, (src, w4) in enumerate(zip(srcs, (w_high, w_low))):

            def put(g, value, number=number):
                walls[2 * side + number, pl.ds(8 * g, 8), :] = value

            tall_window(src, w4, put, PICKS[number][0], tall // 8)
        return carry

    lax.fori_loop(0, 2, vertical, 0)
    block = 104

    def combine(i, carry):
        start = multiple(i, block)
        here = pl.ds(start, block)
        there = pl.ds(start + BORDER, block)
        lane = lane_index(block)
        lh, ll, rh, rl = (walls[number, here, :] for number in range(4))
        body = lane < LANES - BORDER
        h = jnp.maximum(high[0, here, :], jnp.where(body, lh, -BIG))
        l = jnp.minimum(low[0, here, :], jnp.where(body, ll, BIG))
        near = ends[0, here, :] - 0.5 * (h + l)
        body = lane >= BORDER
        h = jnp.maximum(high[1, here, :], jnp.where(body, rh, -BIG))
        l = jnp.minimum(low[1, here, :], jnp.where(body, rl, BIG))
        far = ends[1, here, :] - 0.5 * (h + l)
        mine = lane < LANES // 2
        h = jnp.maximum(high[2, here, :], jnp.where(mine, rh, lh))
        l = jnp.minimum(low[2, here, :], jnp.where(mine, rl, ll))
        strip = pl.ds(start + REACH, block)
        spare = jnp.where(mine, strips[1, strip, :], strips[0, strip, :]) - 0.5 * (h + l)
        inner = beside[here, :]
        wests = [down(t, -1, 1) for t in (near, far, spare, inner)]
        easts = [down(t, 1, 1) for t in (near, far, spare, inner)]

        def west(tile, before):
            return jnp.where(lane == 0, before, wests[tile])

        def east(tile, after):
            return jnp.where(lane == LANES - 1, after, easts[tile])

        for tile, (p, w, e) in enumerate((
            (near, west(0, jnp.where(place.left, near, wests[2])), east(0, easts[3])),
            (far, west(1, wests[3]), east(1, jnp.where(place.right, far, easts[2]))),
            (spare, west(2, wests[1]), east(2, easts[0])),
        )):
            ab[2 * tile, there, :], ab[2 * tile + 1, there, :] = slopes(p, w, e)
        return carry

    lax.fori_loop(0, tall // block, combine, 0)
    fix_rows(ab, 2 * BORDER, rows, place)
    shading(ab, lit, tall, 104)
    send_tile(lit.at[0], 0)
    send_tile(lit.at[1], tiles - 1)
    row_levels(lit, u1, u2, u3, rows, place)

    def level(mine, inner, start, count, m):
        here = pl.ds(start, count)
        parts = [mine[0, here, :]] + [inner[tile, here, :] for tile in range(tiles - 2)] + [mine[1, here, :], mine[2, here, :]]
        return two_pass(jnp.concatenate(parts, axis=1), m[...])

    f1[...] = level(u1, u1_in, 3, rows // 2, c1)
    send(f1, first, tiles)
    f2[...] = level(u2, u2_in, 1, rows // 4, c2)
    send(f2, second, tiles + 1)
    f3[...] = level(u3, u3_in, 0, rows // 8, c3).T[: width // 8]
    send(f3, third, tiles + 2)
    for copy in copies:
        copy.wait()


def on_device(x):
    rows, width = x.shape
    f32, bf16 = jnp.float32, jnp.bfloat16
    tall, deep = rows + 2 * BORDER, rows + 2 * HALO
    most = pl.cdiv(tall, LANES) * LANES
    tiles = width // LANES
    shape = jax.ShapeDtypeStruct
    scratch = lambda *s: pltpu.VMEM(s, f32)

    def call(kernel, ins, outs, scratches, mib, flops, name):
        return pl.pallas_call(
            kernel,
            in_specs=ins,
            out_specs=[VMEM] * len(outs) if name != "late" else [ANY] * len(outs),
            out_shape=[shape(s, t) for s, t in outs],
            scratch_shapes=scratches,
            compiler_params=pltpu.CompilerParams(vmem_limit_bytes=mib * 2**20),
            cost_estimate=pl.CostEstimate(flops=flops, bytes_accessed=8_000_000, transcendentals=0),
        )

    def swap(value, axis, odd):
        count = lax.axis_size(axis)
        pairs = [(i, i + 1) for i in range(1 if odd else 0, count - 1, 2)]
        return lax.ppermute(value, axis, pairs + [(j, i) for i, j in pairs])

    tip, mid = ((2 * HALO, LANES), f32), ((rows - 2 * HALO, LANES), f32)
    edge, corner = ((HALO, width), f32), ((HALO, 2 * LANES), f32)
    sends = call(pack_kernel, [HBM], [tip, tip, mid, mid, edge, edge], [pltpu.SemaphoreType.DMA((8,))], 4, 1000, "pack")(x)
    b_ends = swap(sends[1], "cols", True)
    a_ends = swap(sends[0], "cols", False)
    b_mid = swap(sends[3], "cols", True)
    a_mid = swap(sends[2], "cols", False)
    by_y = swap(sends[4], "rows", True)
    by_core = swap(sends[5], "rows", False)
    to_y, to_core = call(corner_kernel, [VMEM, VMEM], [corner, corner], [], 2, 1000, "corner")(a_ends, b_ends)
    corner_y = swap(to_y, "rows", True)
    corner_core = swap(to_core, "rows", False)

    level_rows = (tall + BORDER, rows // 2 + 3 * BORDER, rows // 4 + 2 * BORDER, rows // 8)
    early = call(
        early_kernel,
        [VMEM] * 3,
        [
            ((3, most, LANES), f32),
            ((3, most, LANES), f32),
            ((2, most, LANES), f32),
            ((most, LANES), f32),
            *(((tiles - 2, n, LANES), f32) for n in level_rows),
            ((width + LANES, width // 2), bf16),
            ((width + LANES, width // 4), bf16),
            ((width + LANES, LANES), bf16),
        ],
        [
            scratch(tiles, deep + 8, LANES),
            scratch(deep + 8, LANES),
            scratch(deep + 8, LANES),
            scratch(tiles, most, LANES),
            scratch(tiles, most, LANES),
            scratch(width + 2 * HALO + 8, LANES),
            scratch(width + 2 * HALO + 8, LANES),
            scratch(width + 2 * BORDER, LANES),
            scratch(width + 2 * BORDER, LANES),
            scratch(2 * (tiles - 2), most + 2 * BORDER, LANES),
        ],
        20,
        80_000_000,
        "early",
    )(x, by_core, by_y)
    *outs, third = call(
        late_kernel,
        [VMEM] * 17,
        [((rows >> k, width >> k), f32) for k in range(3)] + [((width // 8, rows // 8), f32)],
        [
            scratch(2, deep + 8, LANES),
            scratch(4, deep + 8, LANES),
            scratch(4, LANES + 16, LANES),
            scratch(4, LANES + 8, LANES),
            scratch(deep + 8, LANES),
            scratch(deep + 8, LANES),
            scratch(4, tall, LANES),
            scratch(6, tall + 3 * BORDER, LANES),
            *(scratch(3, n, LANES) for n in level_rows),
            scratch(rows // 2, width // 2),
            scratch(rows // 4, width // 4),
            scratch(width // 8, rows // 8),
            pltpu.SemaphoreType.DMA((tiles + 3,)),
        ],
        20,
        80_000_000,
        "late",
    )(a_ends, b_ends, a_mid, b_mid, corner_core, corner_y, *early)
    return (*outs, third.T)


def solution(mesh):
    spec = P("rows", "cols")

    return jax.shard_map(on_device, mesh=mesh, in_specs=(spec,), out_specs=(spec,) * 4, check_vma=False)
```

```python
import math

import jax
import jax.numpy as jnp
import numpy as np
from jax import lax
from jax.experimental import pallas as pl
from jax.experimental.pallas import tpu as pltpu
from jax.sharding import PartitionSpec as P

REACH = 120
HALO = 128
BORDER = 8
LANES = 128
BIG = float("inf")
light_up = math.sqrt(0.5)
VMEM = pl.BlockSpec(memory_space=pltpu.VMEM)
ANY = pl.BlockSpec(memory_space=pl.ANY)
HBM = pl.BlockSpec(memory_space=pltpu.HBM)
SLOTS = 3
PICKS = ((jnp.maximum, -BIG), (jnp.minimum, BIG))


class Place:
    def __init__(self):
        row, col = lax.axis_index("rows"), lax.axis_index("cols")
        self.top, self.bottom = row == 0, row == lax.axis_size("rows") - 1
        self.left, self.right = col == 0, col == lax.axis_size("cols") - 1
        self.even_row, self.even_col = row % 2 == 0, col % 2 == 0


def down(t, shift, axis):
    return pltpu.roll(t, (-shift) % t.shape[axis], axis)


def multiple(i, size):
    return pl.multiple_of(i * size, size)


def fours(srcs, dsts, offset, rows, block, inline=False):
    def step(i, carry):
        start = offset + (i * block if inline else multiple(i, block))
        both = [[src[pl.ds(start + tap, block), :] for tap in range(4)] for src in srcs]
        for (pick, _), (a, b, c, d), dst in zip(PICKS, both * (2 // len(srcs)), dsts):
            dst[pl.ds(start, block), :] = pick(pick(a, b), pick(c, d))
        return carry

    if inline:
        for i in range(rows // block):
            step(i, 0)
    else:
        lax.fori_loop(0, rows // block, step, 0)


def tall_window(src, w4, put, pick, groups, first=0, last=1 << 20):
    levels = [{} for _ in range(5)]

    def join(a, b):
        return a if b is None else b if a is None else pick(a, b)

    def cells(g):
        return src[pl.ds(8 * g, 8), :] if first <= g < last else None

    def eight(g):
        return pick(w4[pl.ds(8 * g, 8), :], w4[pl.ds(8 * g + 4, 8), :]) if first - 1 <= g < last else None

    for g in range(groups + 29):
        levels[0][g] = eight(g)
        at = g
        for level, shift in enumerate((1, 2, 4, 8)):
            at -= shift
            if at >= 0:
                levels[level + 1][at] = join(levels[level].pop(at), levels[level][at + shift])
        out = g - 29
        if out >= 0:
            put(out, join(join(levels[4].pop(out), levels[4][out + 14]), cells(out + 30)))


def tent(in_lanes, out_lanes, in_size, left, right):
    out_size = in_size // 2
    m = np.zeros((in_lanes, out_lanes))
    for lane in range(out_lanes):
        out = lane if lane < out_lanes - LANES // 2 or out_lanes == LANES else lane - out_lanes
        out = max(out, 0) if left else out
        out = min(out, out_size - 1) if right else out
        for tap, weight in enumerate((0.125, 0.375, 0.375, 0.125)):
            col = 2 * out - 1 + tap
            col = max(col, 0) if left else col
            col = min(col, in_size - 1) if right else col
            if -LANES // 2 <= col < in_lanes - LANES // 2:
                m[col % in_lanes, lane] += weight
    return m


def tents(width, left, right):
    m1 = tent(width + LANES, width // 2 + LANES, width, left, right)
    m2 = m1 @ tent(width // 2 + LANES, width // 4 + LANES, width // 2, left, right)
    m3 = m2 @ tent(width // 4 + LANES, LANES, width // 4, left, right)
    parts = (m1[:, : width // 2], m2[:, : width // 4], m3)
    return jnp.concatenate([jnp.asarray(part, jnp.bfloat16) for part in parts], axis=1)


def fix_rows(ref, first, rows, place):
    @pl.when(place.top)
    def _():
        for tile in range(ref.shape[0]):
            ref[tile, pl.ds(first - 1, 1), :] = ref[tile, pl.ds(first, 1), :]

    @pl.when(place.bottom)
    def _():
        for tile in range(ref.shape[0]):
            ref[tile, pl.ds(first + rows, 1), :] = ref[tile, pl.ds(first + rows - 1, 1), :]


def slopes(p, west, east):
    return east - west, (east + west) + (p + p)


def shading(ab, lit, rows, block):
    count = ab.shape[0] // 2

    def step(i, carry):
        start = multiple(i, block)
        for tile in range(count):
            a = ab.at[2 * tile]
            b = ab.at[2 * tile + 1]
            north, here, south = (pl.ds(start + BORDER + shift, block) for shift in (-1, 0, 1))
            mid = a[here, :]
            gx = (a[north, :] + a[south, :]) + (mid + mid)
            gy = b[south, :] - b[north, :]
            lum = (light_up + 0.125 * (gx + gy)) * lax.rsqrt(1.0 + 0.0625 * (gx * gx + gy * gy))
            lit[tile, pl.ds(start, block), :] = jnp.maximum(lum, 0.0)
        return carry

    lax.fori_loop(0, rows // block, step, 0)


def halve_rows(src, dst, start, count):
    for tile in range(src.shape[0]):
        a, b, c, d = (src[tile, pl.ds(start + tap, count, stride=2), :] for tap in range(4))
        dst[tile, pl.ds(0, count), :] = ((a + d) + 3.0 * (b + c)) * 0.125


def row_levels(lit, u1, u2, u3, rows, place):
    fix_rows(lit, BORDER, rows, place)
    halve_rows(lit, u1, 1, rows // 2 + BORDER)
    fix_rows(u1, 3, rows // 2, place)
    halve_rows(u1, u2, 0, rows // 4 + BORDER)
    fix_rows(u2, 1, rows // 4, place)
    halve_rows(u2, u3, 0, rows // 8)


def lane_index(rows):
    return lax.broadcasted_iota(jnp.int32, (rows, LANES), 1)


def pack_kernel(x, a_ends, b_ends, a_mid, b_mid, to_y, to_core, sems):
    place = Place()
    rows, width = x.shape
    far = pl.multiple_of(width - LANES + 0 * lax.axis_index("cols"), LANES)
    a_lanes = pl.ds(pl.multiple_of(jnp.where(place.even_col, far, 0), LANES), LANES)
    b_lanes = pl.ds(pl.multiple_of(jnp.where(place.even_col, 0, far), LANES), LANES)
    low = rows - HALO
    head = a_ends.shape[0] - HALO
    y_rows = pl.ds(pl.multiple_of(jnp.where(place.even_row, 0, low), HALO), HALO)
    core_rows = pl.ds(pl.multiple_of(jnp.where(place.even_row, low, 0), HALO), HALO)
    pairs = []
    for lanes, ends, mid in ((b_lanes, b_ends, b_mid), (a_lanes, a_ends, a_mid)):
        pairs.append((x.at[pl.ds(0, head), lanes], ends.at[pl.ds(0, head), :]))
        pairs.append((x.at[pl.ds(low, HALO), lanes], ends.at[pl.ds(head, HALO), :]))
        pairs.append((x.at[pl.ds(head, low - head), lanes], mid))
    pairs.append((x.at[y_rows, :], to_y))
    pairs.append((x.at[core_rows, :], to_core))
    copies = [pltpu.make_async_copy(src, dst, sems.at[number]) for number, (src, dst) in enumerate(pairs)]
    for copy in copies:
        copy.start()
    for copy in copies:
        copy.wait()


def corner_kernel(a_ends, b_ends, to_y, to_core):
    even_row = Place().even_row
    low = a_ends.shape[0] - HALO
    y_rows = pl.ds(pl.multiple_of(jnp.where(even_row, 0, low), HALO), HALO)
    core_rows = pl.ds(pl.multiple_of(jnp.where(even_row, low, 0), HALO), HALO)
    for number, ends in enumerate((a_ends, b_ends)):
        lanes = pl.ds(number * LANES, LANES)
        to_y[:, lanes] = ends[y_rows, :]
        to_core[:, lanes] = ends[core_rows, :]


def halo_rows(dst, rows, by_core, by_y, first, last, place):
    below = HALO + rows

    @pl.when(jnp.logical_and(place.even_row, jnp.logical_not(place.top)))
    def _():
        dst(0, by_y)

    @pl.when(jnp.logical_not(place.even_row))
    def _():
        dst(0, by_core)

    @pl.when(jnp.logical_and(place.even_row, jnp.logical_not(place.bottom)))
    def _():
        dst(below, by_core)

    @pl.when(jnp.logical_and(jnp.logical_not(place.even_row), jnp.logical_not(place.bottom)))
    def _():
        dst(below, by_y)

    @pl.when(place.top)
    def _():
        dst(0, first)

    @pl.when(place.bottom)
    def _():
        dst(below, last)


def early_kernel(
    x, by_core, by_y,
    high, low, ends, beside, lit, u1, u2, u3,
    xs, w_high, w_low, v_high, v_low, t_high, t_low, q_high, q_low, h_high, h_low, ab,
):
    place = Place()
    rows, width = x.shape
    tiles = width // LANES
    tall, deep = rows + 2 * BORDER, rows + 2 * HALO
    lanes_of = [slice(tile * LANES, (tile + 1) * LANES) for tile in range(tiles)]
    for tile in range(tiles):
        xs[tile, pl.ds(HALO, rows), :] = x[:, lanes_of[tile]]

    def whole_row(start, value):
        for tile in range(tiles):
            xs[tile, pl.ds(start, HALO), :] = jnp.broadcast_to(value[:, lanes_of[tile]], (HALO, LANES))

    halo_rows(whole_row, rows, by_core, by_y, x.at[pl.ds(0, 1), :], x.at[pl.ds(rows - 1, 1), :], place)

    def vertical(tile, carry):
        src = xs.at[tile]
        fours((src,), (w_high, w_low), 0, deep, 80)
        for (pick, _), w4, v in zip(PICKS, (w_high, w_low), (v_high, v_low)):

            def put(g, value, v=v):
                v[tile, pl.ds(8 * g, 8), :] = value

            tall_window(src, w4, put, pick, tall // 8)
        return carry

    lax.fori_loop(0, tiles, vertical, 0)

    for (_, spare), t, w in zip(PICKS, (t_high, t_low), (q_high, q_low)):
        for slot in range(SLOTS):
            for start in (0, HALO + width):
                t[slot, pl.ds(start, HALO), :] = jnp.full((HALO, LANES), spare, jnp.float32)
            w[slot, pl.ds(HALO + width, HALO), :] = jnp.full((HALO, LANES), spare, jnp.float32)

    def block(number, slot):
        at_row = multiple(number, LANES)
        here = pl.ds(at_row, LANES)
        ts, ws, hs = ([pair[0].at[slot], pair[1].at[slot]] for pair in ((t_high, t_low), (q_high, q_low), (h_high, h_low)))
        for v, t in zip((v_high, v_low), ts):
            for tile in range(tiles):
                t[pl.ds(HALO + tile * LANES, LANES), :] = v[tile, here, :].T
        fours(ts, ws, REACH, width + BORDER, 104, inline=True)
        for (pick, _), t, w4, h in zip(PICKS, ts, ws, hs):

            def put(g, value, h=h):
                h[pl.ds(8 * g, 8), :] = value

            tall_window(t, w4, put, pick, (width + 2 * BORDER) // 8, HALO // 8, (HALO + width) // 8)
        own = pl.ds(at_row + REACH, LANES)
        there = pl.ds(at_row + BORDER, LANES)
        p = []
        for tile in range(tiles):
            at = pl.ds(BORDER + tile * LANES, LANES)
            mine = xs[tile, own, :]
            if tile in (0, tiles - 1):
                into = min(tile, 1)
                hi, lo = (h[at, :].T for h in hs)
                high[into, here, :] = hi
                low[into, here, :] = lo
                ends[into, here, :] = mine
                p.append(mine - 0.5 * (hi + lo))
            else:
                p.append(mine - 0.5 * (hs[0][at, :] + hs[1][at, :]).T)
        for h, out in zip(hs, (high, low)):
            t = [h[pl.ds(width + BORDER, BORDER), :], h[pl.ds(2 * BORDER, LANES - 2 * BORDER), :], h[pl.ds(0, BORDER), :]]
            out[2, here, :] = jnp.concatenate(t, axis=0).T
        lane = lane_index(LANES)
        wests = [down(t, -1, 1) for t in p[:-1]]
        easts = [down(t, 1, 1) for t in p[1:]]
        for tile in range(1, tiles - 1):
            w = jnp.where(lane == 0, wests[tile - 1], wests[tile])
            e = jnp.where(lane == LANES - 1, easts[tile], easts[tile - 1])
            ab[2 * tile - 2, there, :], ab[2 * tile - 1, there, :] = slopes(p[tile], w, e)
        beside[here, :] = jnp.where(lane < LANES // 2, wests[tiles - 2], easts[0])

    def columns(i, carry):
        for slot in range(SLOTS):
            block(i * SLOTS + slot, slot)
        return carry

    blocks = pl.cdiv(tall, LANES)
    lax.fori_loop(0, blocks // SLOTS, columns, 0)
    for number in range(blocks // SLOTS * SLOTS, blocks):
        block(number, 0)
    fix_rows(ab, 2 * BORDER, rows, place)
    shading(ab, lit, tall, 104)
    row_levels(lit, u1, u2, u3, rows, place)


def level_parts(width):
    a, b = width // 2, width // 2 + width // 4
    return (3, slice(0, a)), (1, slice(a, b)), (0, slice(b, b + LANES))


def two_pass(t, m):
    rows = t.shape[0]
    head = t.astype(jnp.bfloat16)
    tail = (t - head.astype(jnp.float32)).astype(jnp.bfloat16)
    both = jnp.dot(jnp.concatenate([head, tail], axis=0), m, preferred_element_type=jnp.float32)
    return both[:rows] + both[rows:]


def running(t, work, w4, pick, spare, sign):
    n = t.shape[0] // 8
    order = range(n - 1, -1, -1) if sign > 0 else range(n)
    total = None
    for g in order:
        part = t[8 * g : 8 * g + 8]
        total = part if total is None else pick(total, part)
        work[pl.ds(8 * g + 8, 8), :] = total
    work[pl.ds(8 * n + 8 if sign > 0 else 0, 8), :] = jnp.full((8, t.shape[1]), spare, jnp.float32)
    rows = 8 * n + 8 - 4
    base = 8 if sign > 0 else 1
    a, b, c, d = (work[pl.ds(base + tap, rows), :] for tap in range(4))
    w4[pl.ds(0, rows), :] = pick(pick(a, b), pick(c, d))
    return pick(w4[pl.ds(0, 8 * n), :], w4[pl.ds(4, 8 * n), :])


def scan_block(strips, scans, number, turn, work, w4s, place):
    here = pl.ds(multiple(number, LANES), LANES)
    for side, (sign, gone) in enumerate(((1, place.left), (-1, place.right))):
        t = strips[side, here, :].T
        for kind, (pick, spare) in enumerate(PICKS):
            slot = 2 * side + kind
            spot = 4 * turn + slot
            r = running(jnp.where(gone, spare, t), work.at[spot], w4s.at[spot], pick, spare, sign)
            r = jnp.concatenate([r[BORDER:], r[:BORDER]] if sign > 0 else [r[-BORDER:], r[:-BORDER]], axis=0)
            scans[slot, here, :] = r.T


def middle_kernel(
    a_ends, b_ends, by_core, by_y, u1, u2, u3, weights, weights_left, weights_right,
    strips, scans, c, g1, g2, g3, work, w4s,
):
    place = Place()
    deep = strips.shape[1] - 8
    rows = deep - 2 * HALO
    tiles = u1.shape[0] + 2
    width = tiles * LANES
    head = a_ends.shape[0] - HALO
    for kind, tips in enumerate((a_ends, b_ends)):
        dst = strips.at[jnp.where(place.even_col, 1 - kind, kind)]
        lanes = pl.ds(kind * LANES, LANES)
        dst[pl.ds(HALO, head), :] = tips[pl.ds(0, head), :]
        dst[pl.ds(rows, HALO), :] = tips[pl.ds(head, HALO), :]

        def write(start, value, dst=dst):
            dst[pl.ds(start, HALO), :] = jnp.broadcast_to(value[...], (HALO, LANES))

        edges = (tips.at[pl.ds(0, 1), :], tips.at[pl.ds(head + HALO - 1, 1), :])
        halo_rows(write, rows, by_core.at[:, lanes], by_y.at[:, lanes], *edges, place)
    blocks, ahead = deep // LANES, head // LANES + 1

    def step(i, carry):
        first = 2 * i + jnp.where(i == ahead // 2, blocks - 2 - ahead, 0)
        for turn in range(2):
            scan_block(strips, scans, first + turn, turn, work, w4s, place)
        return carry

    lax.fori_loop(0, ahead // 2 + 1, step, 0)
    c[...] = weights[...]
    few = 2 * BORDER

    @pl.when(place.left)
    def _():
        c[pl.ds(0, few), :] = weights_left[pl.ds(0, few), :]
        c[pl.ds(width + LANES - few, few), :] = weights_left[pl.ds(few, few), :]

    @pl.when(place.right)
    def _():
        c[pl.ds(width - few, 2 * few), :] = weights_right[...]

    for u, g, (start, lanes) in zip((u1, u2, u3), (g1, g2, g3), level_parts(width)):
        here = pl.ds(start, g.shape[0])
        t = jnp.concatenate([u[tile, here, :] for tile in range(tiles - 2)], axis=1)
        g[...] = two_pass(t, c[LANES : width - LANES, lanes])


def late_kernel(
    a_mid, b_mid, strips_in, scans_in, c, g1, g2, g3, high, low, ends, beside, lit_in,
    strips, scans, shade, first, second, third,
    work, w4s, w_high, w_low, walls, ab, lit, u1, u2, u3, f1, f2, f3, sems,
):
    place = Place()
    rows = strips.shape[1] - 8 - 2 * HALO
    head = rows - HALO - a_mid.shape[0]
    tiles = lit_in.shape[0] + 2
    width = tiles * LANES
    tall, deep = rows + 2 * BORDER, rows + 2 * HALO
    copies = []

    def send(src, out, number):
        copies.append(pltpu.make_async_copy(src, out, sems.at[number]))
        copies[-1].start()

    def send_tile(src, tile):
        send(src.at[pl.ds(BORDER, rows), :], shade.at[:, pl.ds(tile * LANES, LANES)], tile)

    for tile in range(1, tiles - 1):
        send_tile(lit_in.at[tile - 1], tile)
    for kind, mid in enumerate((a_mid, b_mid)):
        strips.at[jnp.where(place.even_col, 1 - kind, kind)][pl.ds(HALO + head, mid.shape[0]), :] = mid[...]

    def scan(i, carry):
        for turn in range(2):
            scan_block(strips, scans, head // LANES + 1 + 2 * i + turn, turn, work, w4s, place)
        return carry

    lax.fori_loop(0, a_mid.shape[0] // LANES // 2, scan, 0)

    def vertical(side, carry):
        srcs = (scans.at[2 * side], scans.at[2 * side + 1])
        fours(srcs, (w_high, w_low), 0, deep, 80)
        for number, (src, w4) in enumerate(zip(srcs, (w_high, w_low))):

            def put(g, value, number=number):
                walls[2 * side + number, pl.ds(8 * g, 8), :] = value

            tall_window(src, w4, put, PICKS[number][0], tall // 8)
        return carry

    lax.fori_loop(0, 2, vertical, 0)
    block = 208

    def combine(i, carry):
        start = multiple(i, block)
        here = pl.ds(start, block)
        there = pl.ds(start + BORDER, block)
        lane = lane_index(block)
        lh, ll, rh, rl = (walls[number, here, :] for number in range(4))
        body = lane < LANES - BORDER
        h = jnp.maximum(high[0, here, :], jnp.where(body, lh, -BIG))
        l = jnp.minimum(low[0, here, :], jnp.where(body, ll, BIG))
        near = ends[0, here, :] - 0.5 * (h + l)
        body = lane >= BORDER
        h = jnp.maximum(high[1, here, :], jnp.where(body, rh, -BIG))
        l = jnp.minimum(low[1, here, :], jnp.where(body, rl, BIG))
        far = ends[1, here, :] - 0.5 * (h + l)
        mine = lane < LANES // 2
        h = jnp.maximum(high[2, here, :], jnp.where(mine, rh, lh))
        l = jnp.minimum(low[2, here, :], jnp.where(mine, rl, ll))
        strip = pl.ds(start + REACH, block)
        spare = jnp.where(mine, strips[1, strip, :], strips[0, strip, :]) - 0.5 * (h + l)
        inner = beside[here, :]
        wests = [down(t, -1, 1) for t in (near, far, spare)]
        easts = [down(t, 1, 1) for t in (near, far, spare)]

        def west(tile, before):
            return jnp.where(lane == 0, before, wests[tile])

        def east(tile, after):
            return jnp.where(lane == LANES - 1, after, easts[tile])

        for tile, (p, w, e) in enumerate((
            (near, west(0, jnp.where(place.left, near, wests[2])), east(0, inner)),
            (far, west(1, inner), east(1, jnp.where(place.right, far, easts[2]))),
            (spare, west(2, wests[1]), east(2, easts[0])),
        )):
            ab[2 * tile, there, :], ab[2 * tile + 1, there, :] = slopes(p, w, e)
        return carry

    lax.fori_loop(0, tall // block, combine, 0)
    fix_rows(ab, 2 * BORDER, rows, place)
    shading(ab, lit, tall, 104)
    send_tile(lit.at[0], 0)
    send_tile(lit.at[1], tiles - 1)
    row_levels(lit, u1, u2, u3, rows, place)

    def level(u, inner, number):
        start, lanes = level_parts(width)[number]
        t = jnp.concatenate([u[tile, pl.ds(start, inner.shape[0]), :] for tile in range(3)], axis=1)
        m = jnp.concatenate([c[:LANES, lanes], c[width - LANES :, lanes]], axis=0)
        return inner[...] + two_pass(t, m)

    f1[...] = level(u1, g1, 0)
    send(f1, first, tiles)
    f2[...] = level(u2, g2, 1)
    send(f2, second, tiles + 1)
    f3[...] = level(u3, g3, 2).T[: width // 8]
    send(f3, third, tiles + 2)
    for copy in copies:
        copy.wait()


def on_device(x):
    rows, width = x.shape
    f32, bf16 = jnp.float32, jnp.bfloat16
    tall, deep = rows + 2 * BORDER, rows + 2 * HALO
    most = pl.cdiv(tall, LANES) * LANES
    tiles = width // LANES
    shape = jax.ShapeDtypeStruct
    scratch = lambda *s: pltpu.VMEM(s, f32)

    def call(kernel, ins, outs, scratches, mib, flops, spaces=None, aliases={}):
        return pl.pallas_call(
            kernel,
            in_specs=ins,
            out_specs=spaces or [VMEM] * len(outs),
            input_output_aliases=aliases,
            out_shape=[shape(s, t) for s, t in outs],
            scratch_shapes=scratches,
            compiler_params=pltpu.CompilerParams(vmem_limit_bytes=mib * 2**20),
            cost_estimate=pl.CostEstimate(flops=flops, bytes_accessed=8_000_000, transcendentals=0),
        )

    def swap(value, axis, odd):
        count = lax.axis_size(axis)
        pairs = [(i, i + 1) for i in range(1 if odd else 0, count - 1, 2)]
        return lax.ppermute(value, axis, pairs + [(j, i) for i, j in pairs])

    tip, mid = ((2 * HALO, LANES), f32), ((rows - 2 * HALO, LANES), f32)
    edge, corner = ((HALO, width), f32), ((HALO, 2 * LANES), f32)
    sends = call(pack_kernel, [HBM], [tip, tip, mid, mid, edge, edge], [pltpu.SemaphoreType.DMA((8,))], 4, 1000)(x)
    b_ends = swap(sends[1], "cols", True)
    a_ends = swap(sends[0], "cols", False)
    b_mid = swap(sends[3], "cols", True)
    a_mid = swap(sends[2], "cols", False)
    by_y = swap(sends[4], "rows", True)
    by_core = swap(sends[5], "rows", False)
    to_y, to_core = call(corner_kernel, [VMEM, VMEM], [corner, corner], [], 2, 1000)(a_ends, b_ends)
    corner_y = swap(to_y, "rows", True)
    corner_core = swap(to_core, "rows", False)

    few = 2 * BORDER
    at_left, at_right = tents(width, True, False), tents(width, False, True)
    at_left = jnp.concatenate([at_left[:few], at_left[width + LANES - few :]], axis=0)
    at_right = at_right[width - few : width + few]
    level_rows = (tall + BORDER, rows // 2 + 3 * BORDER, rows // 4 + 2 * BORDER, rows // 8)
    early = call(
        early_kernel,
        [VMEM] * 3,
        [
            ((3, most, LANES), f32),
            ((3, most, LANES), f32),
            ((2, most, LANES), f32),
            ((most, LANES), f32),
            *(((tiles - 2, n, LANES), f32) for n in level_rows),
        ],
        [
            scratch(tiles, deep + 8, LANES),
            scratch(deep + 8, LANES),
            scratch(deep + 8, LANES),
            scratch(tiles, most, LANES),
            scratch(tiles, most, LANES),
            *[scratch(SLOTS, width + 2 * HALO + 8, LANES)] * 4,
            *[scratch(SLOTS, width + 2 * BORDER, LANES)] * 2,
            scratch(2 * (tiles - 2), most + 2 * BORDER, LANES),
        ],
        20,
        80_000_000,
    )(x, by_core, by_y)
    strip, pairs = ((2, deep + 8, LANES), f32), ((4, deep + 8, LANES), f32)
    scanning = [scratch(8, LANES + 16, LANES), scratch(8, LANES + 8, LANES)]
    *early, u1, u2, u3 = early
    parts = [
        ((width + LANES, width // 2 + width // 4 + LANES), bf16),
        ((rows // 2, width // 2), f32),
        ((rows // 4, width // 4), f32),
        ((rows // 8, LANES), f32),
    ]
    middle = call(middle_kernel, [VMEM] * 10, [strip, pairs, *parts], scanning, 8, 10_000_000)(
        a_ends, b_ends, corner_core, corner_y, u1, u2, u3, tents(width, False, False), at_left, at_right
    )
    *outs, third = call(
        late_kernel,
        [VMEM] * 13,
        [strip, pairs] + [((rows >> k, width >> k), f32) for k in range(3)] + [((width // 8, rows // 8), f32)],
        scanning
        + [
            scratch(deep + 8, LANES),
            scratch(deep + 8, LANES),
            scratch(4, tall, LANES),
            scratch(6, tall + 3 * BORDER, LANES),
            *(scratch(3, n, LANES) for n in level_rows),
            scratch(rows // 2, width // 2),
            scratch(rows // 4, width // 4),
            scratch(width // 8, rows // 8),
            pltpu.SemaphoreType.DMA((tiles + 3,)),
        ],
        20,
        80_000_000,
        [VMEM] * 2 + [ANY] * 4,
        {2: 0, 3: 1},
    )(a_mid, b_mid, *middle, *early)
    return (*outs[2:], third.T)


def solution(mesh):
    spec = P("rows", "cols")

    return jax.shard_map(on_device, mesh=mesh, in_specs=(spec,), out_specs=(spec,) * 4, check_vma=False)
```

```python
import math

import jax
import jax.numpy as jnp
import numpy as np
from jax import lax
from jax.experimental import pallas as pl
from jax.experimental.pallas import tpu as pltpu
from jax.sharding import PartitionSpec as P

REACH = 120
HALO = 128
BORDER = 8
LANES = 128
BIG = float("inf")
light_up = math.sqrt(0.5)
VMEM = pl.BlockSpec(memory_space=pltpu.VMEM)
ANY = pl.BlockSpec(memory_space=pl.ANY)
HBM = pl.BlockSpec(memory_space=pltpu.HBM)
SLOTS = 3
TURNS = 3
PICKS = ((jnp.maximum, -BIG), (jnp.minimum, BIG))


class Place:
    def __init__(self):
        row, col = lax.axis_index("rows"), lax.axis_index("cols")
        self.top, self.bottom = row == 0, row == lax.axis_size("rows") - 1
        self.left, self.right = col == 0, col == lax.axis_size("cols") - 1
        self.even_row, self.even_col = row % 2 == 0, col % 2 == 0


def down(t, shift, axis):
    return pltpu.roll(t, (-shift) % t.shape[axis], axis)


def multiple(i, size):
    return pl.multiple_of(i * size, size)


def fours(srcs, dsts, offset, rows, block, inline=False):
    def step(i, carry):
        start = offset + (i * block if inline else multiple(i, block))
        both = [[src[pl.ds(start + tap, block), :] for tap in range(4)] for src in srcs]
        for (pick, _), (a, b, c, d), dst in zip(PICKS, both * (2 // len(srcs)), dsts):
            dst[pl.ds(start, block), :] = pick(pick(a, b), pick(c, d))
        return carry

    if inline:
        for i in range(rows // block):
            step(i, 0)
    else:
        lax.fori_loop(0, rows // block, step, 0)


def tall_window(src, w4, put, pick, groups, first=0, last=1 << 20):
    levels = [{} for _ in range(5)]

    def join(a, b):
        return a if b is None else b if a is None else pick(a, b)

    def cells(g):
        return src[pl.ds(8 * g, 8), :] if first <= g < last else None

    def eight(g):
        return pick(w4[pl.ds(8 * g, 8), :], w4[pl.ds(8 * g + 4, 8), :]) if first - 1 <= g < last else None

    for g in range(groups + 29):
        levels[0][g] = eight(g)
        at = g
        for level, shift in enumerate((1, 2, 4, 8)):
            at -= shift
            if at >= 0:
                levels[level + 1][at] = join(levels[level].pop(at), levels[level][at + shift])
        out = g - 29
        if out >= 0:
            put(out, join(join(levels[4].pop(out), levels[4][out + 14]), cells(out + 30)))


def tent(in_lanes, out_lanes, in_size, left, right):
    out_size = in_size // 2
    m = np.zeros((in_lanes, out_lanes))
    for lane in range(out_lanes):
        out = lane if lane < out_lanes - LANES // 2 or out_lanes == LANES else lane - out_lanes
        out = max(out, 0) if left else out
        out = min(out, out_size - 1) if right else out
        for tap, weight in enumerate((0.125, 0.375, 0.375, 0.125)):
            col = 2 * out - 1 + tap
            col = max(col, 0) if left else col
            col = min(col, in_size - 1) if right else col
            if -LANES // 2 <= col < in_lanes - LANES // 2:
                m[col % in_lanes, lane] += weight
    return m


def tents(width, left, right):
    m1 = tent(width + LANES, width // 2 + LANES, width, left, right)
    m2 = m1 @ tent(width // 2 + LANES, width // 4 + LANES, width // 2, left, right)
    m3 = m2 @ tent(width // 4 + LANES, LANES, width // 4, left, right)
    parts = (m1[:, : width // 2], m2[:, : width // 4], m3)
    return jnp.concatenate([jnp.asarray(part, jnp.bfloat16) for part in parts], axis=1)


def fix_rows(ref, first, rows, place):
    @pl.when(place.top)
    def _():
        for tile in range(ref.shape[0]):
            ref[tile, pl.ds(first - 1, 1), :] = ref[tile, pl.ds(first, 1), :]

    @pl.when(place.bottom)
    def _():
        for tile in range(ref.shape[0]):
            ref[tile, pl.ds(first + rows, 1), :] = ref[tile, pl.ds(first + rows - 1, 1), :]


def slopes(p, west, east):
    return east - west, (east + west) + (p + p)


def shading(ab, lit, rows, block):
    count = ab.shape[0] // 2

    def step(i, carry):
        start = multiple(i, block)
        for tile in range(count):
            a = ab.at[2 * tile]
            b = ab.at[2 * tile + 1]
            north, here, south = (pl.ds(start + BORDER + shift, block) for shift in (-1, 0, 1))
            mid = a[here, :]
            gx = (a[north, :] + a[south, :]) + (mid + mid)
            gy = b[south, :] - b[north, :]
            lum = (light_up + 0.125 * (gx + gy)) * lax.rsqrt(1.0 + 0.0625 * (gx * gx + gy * gy))
            lit[tile, pl.ds(start, block), :] = jnp.maximum(lum, 0.0)
        return carry

    lax.fori_loop(0, rows // block, step, 0)


def halve_rows(src, dst, start, count):
    for tile in range(src.shape[0]):
        a, b, c, d = (src[tile, pl.ds(start + tap, count, stride=2), :] for tap in range(4))
        dst[tile, pl.ds(0, count), :] = ((a + d) + 3.0 * (b + c)) * 0.125


def row_levels(lit, u1, u2, u3, rows, place):
    fix_rows(lit, BORDER, rows, place)
    halve_rows(lit, u1, 1, rows // 2 + BORDER)
    fix_rows(u1, 3, rows // 2, place)
    halve_rows(u1, u2, 0, rows // 4 + BORDER)
    fix_rows(u2, 1, rows // 4, place)
    halve_rows(u2, u3, 0, rows // 8)


def lane_index(rows):
    return lax.broadcasted_iota(jnp.int32, (rows, LANES), 1)


def pack_kernel(x, a_ends, b_ends, a_mid, b_mid, to_y, to_core, sems):
    place = Place()
    rows, width = x.shape
    far = pl.multiple_of(width - LANES + 0 * lax.axis_index("cols"), LANES)
    a_lanes = pl.ds(pl.multiple_of(jnp.where(place.even_col, far, 0), LANES), LANES)
    b_lanes = pl.ds(pl.multiple_of(jnp.where(place.even_col, 0, far), LANES), LANES)
    low = rows - HALO
    head = a_ends.shape[0] - HALO
    y_rows = pl.ds(pl.multiple_of(jnp.where(place.even_row, 0, low), HALO), HALO)
    core_rows = pl.ds(pl.multiple_of(jnp.where(place.even_row, low, 0), HALO), HALO)
    pairs = []
    for lanes, ends, mid in ((b_lanes, b_ends, b_mid), (a_lanes, a_ends, a_mid)):
        pairs.append((x.at[pl.ds(0, head), lanes], ends.at[pl.ds(0, head), :]))
        pairs.append((x.at[pl.ds(low, HALO), lanes], ends.at[pl.ds(head, HALO), :]))
        pairs.append((x.at[pl.ds(head, low - head), lanes], mid))
    pairs.append((x.at[y_rows, :], to_y))
    pairs.append((x.at[core_rows, :], to_core))
    copies = [pltpu.make_async_copy(src, dst, sems.at[number]) for number, (src, dst) in enumerate(pairs)]
    for copy in copies:
        copy.start()
    for copy in copies:
        copy.wait()


def corner_kernel(a_ends, b_ends, to_y, to_core):
    even_row = Place().even_row
    low = a_ends.shape[0] - HALO
    y_rows = pl.ds(pl.multiple_of(jnp.where(even_row, 0, low), HALO), HALO)
    core_rows = pl.ds(pl.multiple_of(jnp.where(even_row, low, 0), HALO), HALO)
    for number, ends in enumerate((a_ends, b_ends)):
        lanes = pl.ds(number * LANES, LANES)
        to_y[:, lanes] = ends[y_rows, :]
        to_core[:, lanes] = ends[core_rows, :]


def halo_rows(dst, rows, by_core, by_y, first, last, place):
    below = HALO + rows

    @pl.when(jnp.logical_and(place.even_row, jnp.logical_not(place.top)))
    def _():
        dst(0, by_y)

    @pl.when(jnp.logical_not(place.even_row))
    def _():
        dst(0, by_core)

    @pl.when(jnp.logical_and(place.even_row, jnp.logical_not(place.bottom)))
    def _():
        dst(below, by_core)

    @pl.when(jnp.logical_and(jnp.logical_not(place.even_row), jnp.logical_not(place.bottom)))
    def _():
        dst(below, by_y)

    @pl.when(place.top)
    def _():
        dst(0, first)

    @pl.when(place.bottom)
    def _():
        dst(below, last)


def early_kernel(
    x, by_core, by_y,
    high, low, xs, beside, lit, u1, u2, u3,
    w_high, w_low, v_high, v_low, t_high, t_low, q_high, q_low, ab,
):
    place = Place()
    rows, width = x.shape
    tiles = width // LANES
    tall, deep = rows + 2 * BORDER, rows + 2 * HALO
    lanes_of = [slice(tile * LANES, (tile + 1) * LANES) for tile in range(tiles)]
    for tile in range(tiles):
        xs[tile, pl.ds(HALO, rows), :] = x[:, lanes_of[tile]]

    def whole_row(start, value):
        for tile in range(tiles):
            xs[tile, pl.ds(start, HALO), :] = jnp.broadcast_to(value[:, lanes_of[tile]], (HALO, LANES))

    halo_rows(whole_row, rows, by_core, by_y, x.at[pl.ds(0, 1), :], x.at[pl.ds(rows - 1, 1), :], place)

    def vertical(tile, carry):
        src = xs.at[tile]
        fours((src,), (w_high, w_low), 0, deep, 160)
        for (pick, _), w4, v in zip(PICKS, (w_high, w_low), (v_high, v_low)):

            def put(g, value, v=v):
                v[tile, pl.ds(8 * g, 8), :] = value

            tall_window(src, w4, put, pick, tall // 8)
        return carry

    lax.fori_loop(0, tiles, vertical, 0)

    for (_, spare), t, w in zip(PICKS, (t_high, t_low), (q_high, q_low)):
        for slot in range(SLOTS):
            for start in (0, HALO + width):
                t[slot, pl.ds(start, HALO), :] = jnp.full((HALO, LANES), spare, jnp.float32)
            w[slot, pl.ds(HALO + width, HALO), :] = jnp.full((HALO, LANES), spare, jnp.float32)

    def block(number, slot):
        at_row = multiple(number, LANES)
        here = pl.ds(at_row, LANES)
        ts, ws = ([pair[0].at[slot], pair[1].at[slot]] for pair in ((t_high, t_low), (q_high, q_low)))
        for v, t in zip((v_high, v_low), ts):
            for tile in range(tiles):
                t[pl.ds(HALO + tile * LANES, LANES), :] = v[tile, here, :].T
        fours(ts, ws, REACH, width + BORDER, 104, inline=True)
        hs = []
        for (pick, _), t, w4 in zip(PICKS, ts, ws):
            hs.append({})
            tall_window(t, w4, hs[-1].__setitem__, pick, (width + 2 * BORDER) // 8, HALO // 8, (HALO + width) // 8)

        def tile_of(h, tile):
            return [h[LANES // 8 * tile + 1 + g] for g in range(LANES // 8)]

        def turned(groups):
            return jnp.concatenate(groups, axis=0).T

        own = pl.ds(at_row + REACH, LANES)
        there = pl.ds(at_row + BORDER, LANES)
        p = []
        for tile in range(tiles):
            mine = xs[tile, own, :]
            if tile in (0, tiles - 1):
                into = min(tile, 1)
                hi, lo = (turned(tile_of(h, tile)) for h in hs)
                high[into, here, :] = hi
                low[into, here, :] = lo
                p.append(mine - 0.5 * (hi + lo))
            else:
                p.append(mine - 0.5 * turned([a + b for a, b in zip(*(tile_of(h, tile) for h in hs))]))
        beyond = (width + BORDER) // 8
        for h, out in zip(hs, (high, low)):
            out[2, here, :] = turned([h[beyond]] * (LANES // 8 - 1) + [h[0]])
        lane = lane_index(LANES)
        wests = [down(t, -1, 1) for t in p[:-1]]
        easts = [down(t, 1, 1) for t in p[1:]]
        for tile in range(1, tiles - 1):
            w = jnp.where(lane == 0, wests[tile - 1], wests[tile])
            e = jnp.where(lane == LANES - 1, easts[tile], easts[tile - 1])
            ab[2 * tile - 2, there, :], ab[2 * tile - 1, there, :] = slopes(p[tile], w, e)
        beside[here, :] = jnp.where(lane < LANES // 2, wests[tiles - 2], easts[0])

    def columns(i, carry):
        for slot in range(SLOTS):
            block(i * SLOTS + slot, slot)
        return carry

    blocks = pl.cdiv(tall, LANES)
    lax.fori_loop(0, blocks // SLOTS, columns, 0)
    for number in range(blocks // SLOTS * SLOTS, blocks):
        block(number, 0)
    fix_rows(ab, 2 * BORDER, rows, place)
    shading(ab, lit, tall, 104)
    row_levels(lit, u1, u2, u3, rows, place)


def level_parts(width):
    a, b = width // 2, width // 2 + width // 4
    return (3, slice(0, a)), (1, slice(a, b)), (0, slice(b, b + LANES))


def two_pass(t, m):
    rows = t.shape[0]
    head = t.astype(jnp.bfloat16)
    tail = (t - head.astype(jnp.float32)).astype(jnp.bfloat16)
    both = jnp.dot(jnp.concatenate([head, tail], axis=0), m, preferred_element_type=jnp.float32)
    return both[:rows] + both[rows:]


def running(t, work, w4, pick, spare, sign):
    n = t.shape[0] // 8
    order = range(n - 1, -1, -1) if sign > 0 else range(n)
    total = None
    for g in order:
        part = t[8 * g : 8 * g + 8]
        total = part if total is None else pick(total, part)
        work[pl.ds(8 * g + 8, 8), :] = total
    work[pl.ds(8 * n + 8 if sign > 0 else 0, 8), :] = jnp.full((8, t.shape[1]), spare, jnp.float32)
    rows = 8 * n + 8 - 4
    base = 8 if sign > 0 else 1
    a, b, c, d = (work[pl.ds(base + tap, rows), :] for tap in range(4))
    w4[pl.ds(0, rows), :] = pick(pick(a, b), pick(c, d))
    return pick(w4[pl.ds(0, 8 * n), :], w4[pl.ds(4, 8 * n), :])


def scan_block(strips, scans, sides, number, turn, work, w4s, place):
    here = pl.ds(multiple(number, LANES), LANES)
    for side in sides:
        sign, gone = ((1, place.left), (-1, place.right))[side]
        t = strips[side, here, :].T
        for kind, (pick, spare) in enumerate(PICKS):
            slot = 2 * side + kind
            spot = 4 * turn + slot
            r = running(jnp.where(gone, spare, t), work.at[spot], w4s.at[spot], pick, spare, sign)
            r = jnp.concatenate([r[BORDER:], r[:BORDER]] if sign > 0 else [r[-BORDER:], r[:-BORDER]], axis=0)
            scans[slot, here, :] = r.T


def finish_side(strips, scans, walls, left, mid, head, work, w4s, w_high, w_low, place):
    deep, tall = strips.shape[1] - 8, walls.shape[1]
    own = jnp.where(left, 0, 1)
    strips.at[own][pl.ds(HALO + head, mid.shape[0]), :] = mid[...]

    def scan(side):
        def step(i, carry):
            for turn in range(TURNS):
                scan_block(strips, scans, (side,), head // LANES + 1 + TURNS * i + turn, turn, work, w4s, place)
            return carry

        lax.fori_loop(0, mid.shape[0] // LANES // TURNS, step, 0)

    pl.when(left)(lambda: scan(0))
    pl.when(jnp.logical_not(left))(lambda: scan(1))
    srcs = (scans.at[2 * own], scans.at[2 * own + 1])
    fours(srcs, (w_high, w_low), 0, deep, 160)
    for number, (src, w4) in enumerate(zip(srcs, (w_high, w_low))):

        def put(g, value, number=number):
            walls[2 * own + number, pl.ds(8 * g, 8), :] = value

        tall_window(src, w4, put, PICKS[number][0], tall // 8)


def middle_kernel(
    a_ends, b_ends, by_core, by_y, b_mid, u1, u2, u3, weights, weights_left, weights_right,
    strips, scans, walls, c, g1, g2, g3, work, w4s, w_high, w_low,
):
    place = Place()
    deep = strips.shape[1] - 8
    rows = deep - 2 * HALO
    tiles = u1.shape[0] + 2
    width = tiles * LANES
    head = a_ends.shape[0] - HALO
    for kind, tips in enumerate((a_ends, b_ends)):
        dst = strips.at[jnp.where(place.even_col, 1 - kind, kind)]
        lanes = pl.ds(kind * LANES, LANES)
        dst[pl.ds(HALO, head), :] = tips[pl.ds(0, head), :]
        dst[pl.ds(rows, HALO), :] = tips[pl.ds(head, HALO), :]

        def write(start, value, dst=dst):
            dst[pl.ds(start, HALO), :] = jnp.broadcast_to(value[...], (HALO, LANES))

        edges = (tips.at[pl.ds(0, 1), :], tips.at[pl.ds(head + HALO - 1, 1), :])
        halo_rows(write, rows, by_core.at[:, lanes], by_y.at[:, lanes], *edges, place)
    blocks, ahead = deep // LANES, head // LANES + 1

    def step(i, carry):
        first = 2 * i + jnp.where(i == ahead // 2, blocks - 2 - ahead, 0)
        for turn in range(2):
            scan_block(strips, scans, (0, 1), first + turn, turn, work, w4s, place)
        return carry

    lax.fori_loop(0, ahead // 2 + 1, step, 0)
    finish_side(strips, scans, walls, place.even_col, b_mid, head, work, w4s, w_high, w_low, place)
    c[...] = weights[...]
    few = 2 * BORDER

    @pl.when(place.left)
    def _():
        c[pl.ds(0, few), :] = weights_left[pl.ds(0, few), :]
        c[pl.ds(width + LANES - few, few), :] = weights_left[pl.ds(few, few), :]

    @pl.when(place.right)
    def _():
        c[pl.ds(width - few, 2 * few), :] = weights_right[...]

    for u, g, (start, lanes) in zip((u1, u2, u3), (g1, g2, g3), level_parts(width)):
        here = pl.ds(start, g.shape[0])
        t = jnp.concatenate([u[tile, here, :] for tile in range(tiles - 2)], axis=1)
        g[...] = two_pass(t, c[LANES : width - LANES, lanes])


def late_kernel(
    a_mid, strips_in, scans_in, walls_in, c, g1, g2, g3, high, low, xs, beside, lit_in,
    strips, scans, walls, shade, first, second, third,
    work, w4s, w_high, w_low, ab, lit, u1, u2, u3, f1, f2, f3, sems,
):
    place = Place()
    rows = strips.shape[1] - 8 - 2 * HALO
    head = rows - HALO - a_mid.shape[0]
    tiles = lit_in.shape[0] + 2
    width = tiles * LANES
    tall = rows + 2 * BORDER
    copies = []

    def send(src, out, number):
        copies.append(pltpu.make_async_copy(src, out, sems.at[number]))
        copies[-1].start()

    def send_tile(src, tile):
        send(src.at[pl.ds(BORDER, rows), :], shade.at[:, pl.ds(tile * LANES, LANES)], tile)

    for tile in range(1, tiles - 1):
        send_tile(lit_in.at[tile - 1], tile)
    finish_side(strips, scans, walls, jnp.logical_not(place.even_col), a_mid, head, work, w4s, w_high, w_low, place)
    block = 520

    def combine(i, carry):
        start = multiple(i, block)
        here = pl.ds(start, block)
        there = pl.ds(start + BORDER, block)
        strip = pl.ds(start + REACH, block)
        lane = lane_index(block)
        lh, ll, rh, rl = (walls[number, here, :] for number in range(4))
        body = lane < LANES - BORDER
        h = jnp.maximum(high[0, here, :], jnp.where(body, lh, -BIG))
        l = jnp.minimum(low[0, here, :], jnp.where(body, ll, BIG))
        near = xs[0, strip, :] - 0.5 * (h + l)
        body = lane >= BORDER
        h = jnp.maximum(high[1, here, :], jnp.where(body, rh, -BIG))
        l = jnp.minimum(low[1, here, :], jnp.where(body, rl, BIG))
        far = xs[tiles - 1, strip, :] - 0.5 * (h + l)
        mine = lane < LANES // 2
        h = jnp.maximum(high[2, here, :], jnp.where(mine, rh, lh))
        l = jnp.minimum(low[2, here, :], jnp.where(mine, rl, ll))
        spare = jnp.where(mine, strips[1, strip, :], strips[0, strip, :]) - 0.5 * (h + l)
        inner = beside[here, :]
        wests = [down(t, -1, 1) for t in (near, far, spare)]
        easts = [down(t, 1, 1) for t in (near, far, spare)]

        def west(tile, before):
            return jnp.where(lane == 0, before, wests[tile])

        def east(tile, after):
            return jnp.where(lane == LANES - 1, after, easts[tile])

        for tile, (p, w, e) in enumerate((
            (near, west(0, jnp.where(place.left, near, wests[2])), east(0, inner)),
            (far, west(1, inner), east(1, jnp.where(place.right, far, easts[2]))),
            (spare, west(2, wests[1]), east(2, easts[0])),
        )):
            ab[2 * tile, there, :], ab[2 * tile + 1, there, :] = slopes(p, w, e)
        return carry

    lax.fori_loop(0, tall // block, combine, 0)
    fix_rows(ab, 2 * BORDER, rows, place)
    shading(ab, lit, tall, 104)
    send_tile(lit.at[0], 0)
    send_tile(lit.at[1], tiles - 1)
    row_levels(lit, u1, u2, u3, rows, place)

    def level(u, inner, number):
        start, lanes = level_parts(width)[number]
        t = jnp.concatenate([u[tile, pl.ds(start, inner.shape[0]), :] for tile in range(3)], axis=1)
        m = jnp.concatenate([c[:LANES, lanes], c[width - LANES :, lanes]], axis=0)
        return inner[...] + two_pass(t, m)

    f1[...] = level(u1, g1, 0)
    send(f1, first, tiles)
    f2[...] = level(u2, g2, 1)
    send(f2, second, tiles + 1)
    f3[...] = level(u3, g3, 2).T[: width // 8]
    send(f3, third, tiles + 2)
    for copy in copies:
        copy.wait()


def on_device(x):
    rows, width = x.shape
    f32, bf16 = jnp.float32, jnp.bfloat16
    tall, deep = rows + 2 * BORDER, rows + 2 * HALO
    most = pl.cdiv(tall, LANES) * LANES
    tiles = width // LANES
    shape = jax.ShapeDtypeStruct
    scratch = lambda *s: pltpu.VMEM(s, f32)

    def call(kernel, ins, outs, scratches, mib, flops, spaces=None, aliases={}):
        return pl.pallas_call(
            kernel,
            in_specs=ins,
            out_specs=spaces or [VMEM] * len(outs),
            input_output_aliases=aliases,
            out_shape=[shape(s, t) for s, t in outs],
            scratch_shapes=scratches,
            compiler_params=pltpu.CompilerParams(vmem_limit_bytes=mib * 2**20),
            cost_estimate=pl.CostEstimate(flops=flops, bytes_accessed=8_000_000, transcendentals=0),
        )

    def swap(value, axis, odd):
        count = lax.axis_size(axis)
        pairs = [(i, i + 1) for i in range(1 if odd else 0, count - 1, 2)]
        return lax.ppermute(value, axis, pairs + [(j, i) for i, j in pairs])

    tip, mid = ((2 * HALO, LANES), f32), ((rows - 2 * HALO, LANES), f32)
    edge, corner = ((HALO, width), f32), ((HALO, 2 * LANES), f32)
    sends = call(pack_kernel, [HBM], [tip, tip, mid, mid, edge, edge], [pltpu.SemaphoreType.DMA((8,))], 52, 1000)(x)
    b_ends = swap(sends[1], "cols", True)
    a_ends = swap(sends[0], "cols", False)
    b_mid = swap(sends[3], "cols", True)
    a_mid = swap(sends[2], "cols", False)
    by_y = swap(sends[4], "rows", True)
    by_core = swap(sends[5], "rows", False)
    to_y, to_core = call(corner_kernel, [VMEM, VMEM], [corner, corner], [], 2, 1000)(a_ends, b_ends)
    corner_y = swap(to_y, "rows", True)
    corner_core = swap(to_core, "rows", False)

    few = 2 * BORDER
    at_left, at_right = tents(width, True, False), tents(width, False, True)
    at_left = jnp.concatenate([at_left[:few], at_left[width + LANES - few :]], axis=0)
    at_right = at_right[width - few : width + few]
    level_rows = (tall + BORDER, rows // 2 + 3 * BORDER, rows // 4 + 2 * BORDER, rows // 8)
    early = call(
        early_kernel,
        [VMEM] * 3,
        [
            ((3, most, LANES), f32),
            ((3, most, LANES), f32),
            ((tiles, deep + 8, LANES), f32),
            ((most, LANES), f32),
            *(((tiles - 2, n, LANES), f32) for n in level_rows),
        ],
        [
            scratch(deep + 8, LANES),
            scratch(deep + 8, LANES),
            scratch(tiles, most, LANES),
            scratch(tiles, most, LANES),
            *[scratch(SLOTS, width + 2 * HALO + 8, LANES)] * 4,
            scratch(2 * (tiles - 2), most + 2 * BORDER, LANES),
        ],
        20,
        80_000_000,
    )(x, by_core, by_y)
    strip, pairs = ((2, deep + 8, LANES), f32), ((4, deep + 8, LANES), f32)
    scanning = [scratch(4 * TURNS, LANES + 16, LANES), scratch(4 * TURNS, LANES + 8, LANES), *[scratch(deep + 8, LANES)] * 2]
    wall = ((4, tall, LANES), f32)
    *early, u1, u2, u3 = early
    parts = [
        ((width + LANES, width // 2 + width // 4 + LANES), bf16),
        ((rows // 2, width // 2), f32),
        ((rows // 4, width // 4), f32),
        ((rows // 8, LANES), f32),
    ]
    middle = call(middle_kernel, [VMEM] * 11, [strip, pairs, wall, *parts], scanning, 8, 10_000_000)(
        a_ends, b_ends, corner_core, corner_y, b_mid, u1, u2, u3, tents(width, False, False), at_left, at_right
    )
    *outs, third = call(
        late_kernel,
        [VMEM] * 13,
        [strip, pairs, wall] + [((rows >> k, width >> k), f32) for k in range(3)] + [((width // 8, rows // 8), f32)],
        scanning
        + [
            scratch(6, tall + 3 * BORDER, LANES),
            *(scratch(3, n, LANES) for n in level_rows),
            scratch(rows // 2, width // 2),
            scratch(rows // 4, width // 4),
            scratch(width // 8, rows // 8),
            pltpu.SemaphoreType.DMA((tiles + 3,)),
        ],
        20,
        80_000_000,
        [VMEM] * 3 + [ANY] * 4,
        {1: 0, 2: 1, 3: 2},
    )(a_mid, *middle, *early)
    return (*outs[3:], third.T)


def solution(mesh):
    spec = P("rows", "cols")

    return jax.shard_map(on_device, mesh=mesh, in_specs=(spec,), out_specs=(spec,) * 4, check_vma=False)
```

```python
import math

import jax
import jax.numpy as jnp
import numpy as np
from jax import lax
from jax.experimental import pallas as pl
from jax.experimental.pallas import tpu as pltpu
from jax.sharding import PartitionSpec as P

REACH = 120
HALO = 128
BORDER = 8
LANES = 128
BIG = float("inf")
light_up = math.sqrt(0.5)
VMEM = pl.BlockSpec(memory_space=pltpu.VMEM)
ANY = pl.BlockSpec(memory_space=pl.ANY)
HBM = pl.BlockSpec(memory_space=pltpu.HBM)
SLOTS = 3
TURNS = 3
PICKS = ((jnp.maximum, -BIG), (jnp.minimum, BIG))


class Place:
    def __init__(self):
        row, col = lax.axis_index("rows"), lax.axis_index("cols")
        self.top, self.bottom = row == 0, row == lax.axis_size("rows") - 1
        self.left, self.right = col == 0, col == lax.axis_size("cols") - 1
        self.even_row, self.even_col = row % 2 == 0, col % 2 == 0


def down(t, shift, axis):
    return pltpu.roll(t, (-shift) % t.shape[axis], axis)


def multiple(i, size):
    return pl.multiple_of(i * size, size)


def fours(srcs, dsts, offset, rows, block, inline=False):
    def step(i, carry):
        start = offset + (i * block if inline else multiple(i, block))
        both = [[src[pl.ds(start + tap, block), :] for tap in range(4)] for src in srcs]
        for (pick, _), (a, b, c, d), dst in zip(PICKS, both * (2 // len(srcs)), dsts):
            dst[pl.ds(start, block), :] = pick(pick(a, b), pick(c, d))
        return carry

    if inline:
        for i in range(rows // block):
            step(i, 0)
    else:
        lax.fori_loop(0, rows // block, step, 0)


def tall_window(src, w4, put, pick, groups, first=0, last=1 << 20):
    levels = [{} for _ in range(5)]

    def join(a, b):
        return a if b is None else b if a is None else pick(a, b)

    def cells(g):
        return src[pl.ds(8 * g, 8), :] if first <= g < last else None

    def eight(g):
        return pick(w4[pl.ds(8 * g, 8), :], w4[pl.ds(8 * g + 4, 8), :]) if first - 1 <= g < last else None

    for g in range(groups + 29):
        levels[0][g] = eight(g)
        at = g
        for level, shift in enumerate((1, 2, 4, 8)):
            at -= shift
            if at >= 0:
                levels[level + 1][at] = join(levels[level].pop(at), levels[level][at + shift])
        out = g - 29
        if out >= 0:
            put(out, join(join(levels[4].pop(out), levels[4][out + 14]), cells(out + 30)))


def tent(in_lanes, out_lanes, in_size, left, right):
    out_size = in_size // 2
    m = np.zeros((in_lanes, out_lanes))
    for lane in range(out_lanes):
        out = lane if lane < out_lanes - LANES // 2 or out_lanes == LANES else lane - out_lanes
        out = max(out, 0) if left else out
        out = min(out, out_size - 1) if right else out
        for tap, weight in enumerate((0.125, 0.375, 0.375, 0.125)):
            col = 2 * out - 1 + tap
            col = max(col, 0) if left else col
            col = min(col, in_size - 1) if right else col
            if -LANES // 2 <= col < in_lanes - LANES // 2:
                m[col % in_lanes, lane] += weight
    return m


def tents(width, left, right):
    m1 = tent(width + LANES, width // 2 + LANES, width, left, right)
    m2 = m1 @ tent(width // 2 + LANES, width // 4 + LANES, width // 2, left, right)
    m3 = m2 @ tent(width // 4 + LANES, LANES, width // 4, left, right)
    parts = (m1[:, : width // 2], m2[:, : width // 4], m3)
    return jnp.concatenate([jnp.asarray(part, jnp.bfloat16) for part in parts], axis=1)


def fix_rows(ref, first, rows, place):
    @pl.when(place.top)
    def _():
        for tile in range(ref.shape[0]):
            ref[tile, pl.ds(first - 1, 1), :] = ref[tile, pl.ds(first, 1), :]

    @pl.when(place.bottom)
    def _():
        for tile in range(ref.shape[0]):
            ref[tile, pl.ds(first + rows, 1), :] = ref[tile, pl.ds(first + rows - 1, 1), :]


def slopes(p, west, east):
    return east - west, (east + west) + (p + p)


def shading(ab, lit, rows, block):
    count = ab.shape[0] // 2

    def step(i, carry):
        start = multiple(i, block)
        for tile in range(count):
            a = ab.at[2 * tile]
            b = ab.at[2 * tile + 1]
            north, here, south = (pl.ds(start + BORDER + shift, block) for shift in (-1, 0, 1))
            mid = a[here, :]
            gx = (a[north, :] + a[south, :]) + (mid + mid)
            gy = b[south, :] - b[north, :]
            lum = (light_up + 0.125 * (gx + gy)) * lax.rsqrt(1.0 + 0.0625 * (gx * gx + gy * gy))
            lit[tile, pl.ds(start, block), :] = jnp.maximum(lum, 0.0)
        return carry

    lax.fori_loop(0, rows // block, step, 0)


def halve_rows(src, dst, start, count):
    for tile in range(src.shape[0]):
        a, b, c, d = (src[tile, pl.ds(start + tap, count, stride=2), :] for tap in range(4))
        dst[tile, pl.ds(0, count), :] = ((a + d) + 3.0 * (b + c)) * 0.125


def row_levels(lit, u1, u2, u3, rows, place):
    fix_rows(lit, BORDER, rows, place)
    halve_rows(lit, u1, 1, rows // 2 + BORDER)
    fix_rows(u1, 3, rows // 2, place)
    halve_rows(u1, u2, 0, rows // 4 + BORDER)
    fix_rows(u2, 1, rows // 4, place)
    halve_rows(u2, u3, 0, rows // 8)


def lane_index(rows):
    return lax.broadcasted_iota(jnp.int32, (rows, LANES), 1)


def pack_kernel(x, a_ends, b_ends, a_mid, b_mid, to_y, to_core, sems):
    place = Place()
    rows, width = x.shape
    far = pl.multiple_of(width - LANES + 0 * lax.axis_index("cols"), LANES)
    a_lanes = pl.ds(pl.multiple_of(jnp.where(place.even_col, far, 0), LANES), LANES)
    b_lanes = pl.ds(pl.multiple_of(jnp.where(place.even_col, 0, far), LANES), LANES)
    low = rows - HALO
    head = a_ends.shape[0] - HALO
    y_rows = pl.ds(pl.multiple_of(jnp.where(place.even_row, 0, low), HALO), HALO)
    core_rows = pl.ds(pl.multiple_of(jnp.where(place.even_row, low, 0), HALO), HALO)
    pairs = []
    for lanes, ends, mid in ((b_lanes, b_ends, b_mid), (a_lanes, a_ends, a_mid)):
        pairs.append((x.at[pl.ds(0, head), lanes], ends.at[pl.ds(0, head), :]))
        pairs.append((x.at[pl.ds(low, HALO), lanes], ends.at[pl.ds(head, HALO), :]))
        pairs.append((x.at[pl.ds(head, low - head), lanes], mid))
    pairs.append((x.at[y_rows, :], to_y))
    pairs.append((x.at[core_rows, :], to_core))
    copies = [pltpu.make_async_copy(src, dst, sems.at[number]) for number, (src, dst) in enumerate(pairs)]
    for copy in copies:
        copy.start()
    for copy in copies:
        copy.wait()


def corner_kernel(a_ends, b_ends, to_y, to_core):
    even_row = Place().even_row
    low = a_ends.shape[0] - HALO
    y_rows = pl.ds(pl.multiple_of(jnp.where(even_row, 0, low), HALO), HALO)
    core_rows = pl.ds(pl.multiple_of(jnp.where(even_row, low, 0), HALO), HALO)
    for number, ends in enumerate((a_ends, b_ends)):
        lanes = pl.ds(number * LANES, LANES)
        to_y[:, lanes] = ends[y_rows, :]
        to_core[:, lanes] = ends[core_rows, :]


def halo_rows(dst, rows, by_core, by_y, first, last, place):
    below = HALO + rows

    @pl.when(jnp.logical_and(place.even_row, jnp.logical_not(place.top)))
    def _():
        dst(0, by_y)

    @pl.when(jnp.logical_not(place.even_row))
    def _():
        dst(0, by_core)

    @pl.when(jnp.logical_and(place.even_row, jnp.logical_not(place.bottom)))
    def _():
        dst(below, by_core)

    @pl.when(jnp.logical_and(jnp.logical_not(place.even_row), jnp.logical_not(place.bottom)))
    def _():
        dst(below, by_y)

    @pl.when(place.top)
    def _():
        dst(0, first)

    @pl.when(place.bottom)
    def _():
        dst(below, last)


def early_kernel(
    x, by_core, by_y,
    high, low, xs, beside, lit, u1, u2, u3,
    w_high, w_low, v_high, v_low, t_high, t_low, q_high, q_low, ab, sems,
):
    place = Place()
    rows, width = x.shape
    tiles = width // LANES
    tall, deep = rows + 2 * BORDER, rows + 2 * HALO
    lanes_of = [slice(tile * LANES, (tile + 1) * LANES) for tile in range(tiles)]

    def own_rows(tile):
        src = x.at[:, pl.ds(multiple(tile, LANES), LANES)]
        return pltpu.make_async_copy(src, xs.at[tile, pl.ds(HALO, rows), :], sems.at[tile])

    for tile in range(tiles):
        own_rows(jnp.int32(tile)).start()

    def whole_row(start, value):
        for tile in range(tiles):
            xs[tile, pl.ds(start, HALO), :] = jnp.broadcast_to(value[:, lanes_of[tile]], (HALO, LANES))

    halo_rows(whole_row, rows, by_core, by_y, x.at[pl.ds(0, 1), :], x.at[pl.ds(rows - 1, 1), :], place)

    def vertical(tile, carry):
        own_rows(tile).wait()
        src = xs.at[tile]
        fours((src,), (w_high, w_low), 0, deep, 160)
        for (pick, _), w4, v in zip(PICKS, (w_high, w_low), (v_high, v_low)):

            def put(g, value, v=v):
                v[tile, pl.ds(8 * g, 8), :] = value

            tall_window(src, w4, put, pick, tall // 8)
        return carry

    lax.fori_loop(0, tiles, vertical, 0)

    for (_, spare), t, w in zip(PICKS, (t_high, t_low), (q_high, q_low)):
        for slot in range(SLOTS):
            for start in (0, HALO + width):
                t[slot, pl.ds(start, HALO), :] = jnp.full((HALO, LANES), spare, jnp.float32)
            w[slot, pl.ds(HALO + width, HALO), :] = jnp.full((HALO, LANES), spare, jnp.float32)

    def block(number, slot):
        at_row = multiple(number, LANES)
        here = pl.ds(at_row, LANES)
        ts, ws = ([pair[0].at[slot], pair[1].at[slot]] for pair in ((t_high, t_low), (q_high, q_low)))
        for v, t in zip((v_high, v_low), ts):
            for tile in range(tiles):
                t[pl.ds(HALO + tile * LANES, LANES), :] = v[tile, here, :].T
        fours(ts, ws, REACH, width + BORDER, 104, inline=True)
        hs = []
        for (pick, _), t, w4 in zip(PICKS, ts, ws):
            hs.append({})
            tall_window(t, w4, hs[-1].__setitem__, pick, (width + 2 * BORDER) // 8, HALO // 8, (HALO + width) // 8)

        def tile_of(h, tile):
            return [h[LANES // 8 * tile + 1 + g] for g in range(LANES // 8)]

        def turned(groups):
            return jnp.concatenate(groups, axis=0).T

        own = pl.ds(at_row + REACH, LANES)
        there = pl.ds(at_row + BORDER, LANES)
        p = []
        for tile in range(tiles):
            mine = xs[tile, own, :]
            if tile in (0, tiles - 1):
                into = min(tile, 1)
                hi, lo = (turned(tile_of(h, tile)) for h in hs)
                high[into, here, :] = hi
                low[into, here, :] = lo
                p.append(mine - 0.5 * (hi + lo))
            else:
                p.append(mine - 0.5 * turned([a + b for a, b in zip(*(tile_of(h, tile) for h in hs))]))
        beyond = (width + BORDER) // 8
        for h, out in zip(hs, (high, low)):
            out[2, here, :] = turned([h[beyond]] * (LANES // 8 - 1) + [h[0]])
        lane = lane_index(LANES)
        wests = [down(t, -1, 1) for t in p[:-1]]
        easts = [down(t, 1, 1) for t in p[1:]]
        for tile in range(1, tiles - 1):
            w = jnp.where(lane == 0, wests[tile - 1], wests[tile])
            e = jnp.where(lane == LANES - 1, easts[tile], easts[tile - 1])
            ab[2 * tile - 2, there, :], ab[2 * tile - 1, there, :] = slopes(p[tile], w, e)
        beside[here, :] = jnp.where(lane < LANES // 2, wests[tiles - 2], easts[0])

    def columns(i, carry):
        for slot in range(SLOTS):
            block(i * SLOTS + slot, slot)
        return carry

    blocks = pl.cdiv(tall, LANES)
    lax.fori_loop(0, blocks // SLOTS, columns, 0)
    for number in range(blocks // SLOTS * SLOTS, blocks):
        block(number, 0)
    fix_rows(ab, 2 * BORDER, rows, place)
    shading(ab, lit, tall, 104)
    row_levels(lit, u1, u2, u3, rows, place)


def level_parts(width):
    a, b = width // 2, width // 2 + width // 4
    return (3, slice(0, a)), (1, slice(a, b)), (0, slice(b, b + LANES))


def two_pass(t, m):
    rows = t.shape[0]
    head = t.astype(jnp.bfloat16)
    tail = (t - head.astype(jnp.float32)).astype(jnp.bfloat16)
    both = jnp.dot(jnp.concatenate([head, tail], axis=0), m, preferred_element_type=jnp.float32)
    return both[:rows] + both[rows:]


def running(t, work, w4, pick, spare, sign):
    n = t.shape[0] // 8
    order = range(n - 1, -1, -1) if sign > 0 else range(n)
    total = None
    for g in order:
        part = t[8 * g : 8 * g + 8]
        total = part if total is None else pick(total, part)
        work[pl.ds(8 * g + 8, 8), :] = total
    work[pl.ds(8 * n + 8 if sign > 0 else 0, 8), :] = jnp.full((8, t.shape[1]), spare, jnp.float32)
    rows = 8 * n + 8 - 4
    base = 8 if sign > 0 else 1
    a, b, c, d = (work[pl.ds(base + tap, rows), :] for tap in range(4))
    w4[pl.ds(0, rows), :] = pick(pick(a, b), pick(c, d))
    return pick(w4[pl.ds(0, 8 * n), :], w4[pl.ds(4, 8 * n), :])


def scan_block(strips, scans, sides, number, turn, work, w4s, place):
    here = pl.ds(multiple(number, LANES), LANES)
    for side in sides:
        sign, gone = ((1, place.left), (-1, place.right))[side]
        t = strips[side, here, :].T
        for kind, (pick, spare) in enumerate(PICKS):
            slot = 2 * side + kind
            spot = 4 * turn + slot
            r = running(jnp.where(gone, spare, t), work.at[spot], w4s.at[spot], pick, spare, sign)
            r = jnp.concatenate([r[BORDER:], r[:BORDER]] if sign > 0 else [r[-BORDER:], r[:-BORDER]], axis=0)
            scans[slot, here, :] = r.T


def finish_side(strips, scans, walls, left, mid, head, work, w4s, w_high, w_low, place):
    deep, tall = strips.shape[1] - 8, walls.shape[1]
    own = jnp.where(left, 0, 1)
    strips.at[own][pl.ds(HALO + head, mid.shape[0]), :] = mid[...]

    def scan(side):
        def step(i, carry):
            for turn in range(TURNS):
                scan_block(strips, scans, (side,), head // LANES + 1 + TURNS * i + turn, turn, work, w4s, place)
            return carry

        lax.fori_loop(0, mid.shape[0] // LANES // TURNS, step, 0)

    pl.when(left)(lambda: scan(0))
    pl.when(jnp.logical_not(left))(lambda: scan(1))
    srcs = (scans.at[2 * own], scans.at[2 * own + 1])
    fours(srcs, (w_high, w_low), 0, deep, 160)
    for number, (src, w4) in enumerate(zip(srcs, (w_high, w_low))):

        def put(g, value, number=number):
            walls[2 * own + number, pl.ds(8 * g, 8), :] = value

        tall_window(src, w4, put, PICKS[number][0], tall // 8)


def middle_kernel(
    a_ends, b_ends, by_core, by_y, b_mid, u1, u2, u3, weights, weights_left, weights_right,
    strips, scans, walls, c, g1, g2, g3, work, w4s, w_high, w_low,
):
    place = Place()
    deep = strips.shape[1] - 8
    rows = deep - 2 * HALO
    tiles = u1.shape[0] + 2
    width = tiles * LANES
    head = a_ends.shape[0] - HALO
    for kind, tips in enumerate((a_ends, b_ends)):
        dst = strips.at[jnp.where(place.even_col, 1 - kind, kind)]
        lanes = pl.ds(kind * LANES, LANES)
        dst[pl.ds(HALO, head), :] = tips[pl.ds(0, head), :]
        dst[pl.ds(rows, HALO), :] = tips[pl.ds(head, HALO), :]

        def write(start, value, dst=dst):
            dst[pl.ds(start, HALO), :] = jnp.broadcast_to(value[...], (HALO, LANES))

        edges = (tips.at[pl.ds(0, 1), :], tips.at[pl.ds(head + HALO - 1, 1), :])
        halo_rows(write, rows, by_core.at[:, lanes], by_y.at[:, lanes], *edges, place)
    blocks, ahead = deep // LANES, head // LANES + 1

    def step(i, carry):
        first = 2 * i + jnp.where(i == ahead // 2, blocks - 2 - ahead, 0)
        for turn in range(2):
            scan_block(strips, scans, (0, 1), first + turn, turn, work, w4s, place)
        return carry

    lax.fori_loop(0, ahead // 2 + 1, step, 0)
    finish_side(strips, scans, walls, place.even_col, b_mid, head, work, w4s, w_high, w_low, place)
    c[...] = weights[...]
    few = 2 * BORDER

    @pl.when(place.left)
    def _():
        c[pl.ds(0, few), :] = weights_left[pl.ds(0, few), :]
        c[pl.ds(width + LANES - few, few), :] = weights_left[pl.ds(few, few), :]

    @pl.when(place.right)
    def _():
        c[pl.ds(width - few, 2 * few), :] = weights_right[...]

    for u, g, (start, lanes) in zip((u1, u2, u3), (g1, g2, g3), level_parts(width)):
        here = pl.ds(start, g.shape[0])
        t = jnp.concatenate([u[tile, here, :] for tile in range(tiles - 2)], axis=1)
        g[...] = two_pass(t, c[LANES : width - LANES, lanes])


def late_kernel(
    a_mid, strips_in, scans_in, walls_in, c, g1, g2, g3, high, low, xs, beside, lit_in,
    strips, scans, walls, shade, first, second, third,
    work, w4s, w_high, w_low, ab, lit, u1, u2, u3, f1, f2, f3, sems,
):
    place = Place()
    rows = strips.shape[1] - 8 - 2 * HALO
    head = rows - HALO - a_mid.shape[0]
    tiles = lit_in.shape[0] + 2
    width = tiles * LANES
    tall = rows + 2 * BORDER
    copies = []

    def send(src, out, number):
        copies.append(pltpu.make_async_copy(src, out, sems.at[number]))
        copies[-1].start()

    def send_tile(src, tile):
        send(src.at[pl.ds(BORDER, rows), :], shade.at[:, pl.ds(tile * LANES, LANES)], tile)

    for tile in range(1, tiles - 1):
        send_tile(lit_in.at[tile - 1], tile)
    finish_side(strips, scans, walls, jnp.logical_not(place.even_col), a_mid, head, work, w4s, w_high, w_low, place)
    block = 520

    def combine(i, carry):
        start = multiple(i, block)
        here = pl.ds(start, block)
        there = pl.ds(start + BORDER, block)
        strip = pl.ds(start + REACH, block)
        lane = lane_index(block)
        lh, ll, rh, rl = (walls[number, here, :] for number in range(4))
        body = lane < LANES - BORDER
        h = jnp.maximum(high[0, here, :], jnp.where(body, lh, -BIG))
        l = jnp.minimum(low[0, here, :], jnp.where(body, ll, BIG))
        near = xs[0, strip, :] - 0.5 * (h + l)
        body = lane >= BORDER
        h = jnp.maximum(high[1, here, :], jnp.where(body, rh, -BIG))
        l = jnp.minimum(low[1, here, :], jnp.where(body, rl, BIG))
        far = xs[tiles - 1, strip, :] - 0.5 * (h + l)
        mine = lane < LANES // 2
        h = jnp.maximum(high[2, here, :], jnp.where(mine, rh, lh))
        l = jnp.minimum(low[2, here, :], jnp.where(mine, rl, ll))
        spare = jnp.where(mine, strips[1, strip, :], strips[0, strip, :]) - 0.5 * (h + l)
        inner = beside[here, :]
        wests = [down(t, -1, 1) for t in (near, far, spare)]
        easts = [down(t, 1, 1) for t in (near, far, spare)]

        def west(tile, before):
            return jnp.where(lane == 0, before, wests[tile])

        def east(tile, after):
            return jnp.where(lane == LANES - 1, after, easts[tile])

        for tile, (p, w, e) in enumerate((
            (near, west(0, jnp.where(place.left, near, wests[2])), east(0, inner)),
            (far, west(1, inner), east(1, jnp.where(place.right, far, easts[2]))),
            (spare, west(2, wests[1]), east(2, easts[0])),
        )):
            ab[2 * tile, there, :], ab[2 * tile + 1, there, :] = slopes(p, w, e)
        return carry

    lax.fori_loop(0, tall // block, combine, 0)
    fix_rows(ab, 2 * BORDER, rows, place)
    shading(ab, lit, tall, 104)
    send_tile(lit.at[0], 0)
    send_tile(lit.at[1], tiles - 1)
    row_levels(lit, u1, u2, u3, rows, place)

    def level(u, inner, number):
        start, lanes = level_parts(width)[number]
        t = jnp.concatenate([u[tile, pl.ds(start, inner.shape[0]), :] for tile in range(3)], axis=1)
        m = jnp.concatenate([c[:LANES, lanes], c[width - LANES :, lanes]], axis=0)
        return inner[...] + two_pass(t, m)

    f1[...] = level(u1, g1, 0)
    send(f1, first, tiles)
    f2[...] = level(u2, g2, 1)
    send(f2, second, tiles + 1)
    f3[...] = level(u3, g3, 2).T[: width // 8]
    send(f3, third, tiles + 2)
    for copy in copies:
        copy.wait()


def on_device(x):
    rows, width = x.shape
    f32, bf16 = jnp.float32, jnp.bfloat16
    tall, deep = rows + 2 * BORDER, rows + 2 * HALO
    most = pl.cdiv(tall, LANES) * LANES
    tiles = width // LANES
    shape = jax.ShapeDtypeStruct
    scratch = lambda *s: pltpu.VMEM(s, f32)

    def call(kernel, ins, outs, scratches, mib, flops, spaces=None, aliases={}):
        return pl.pallas_call(
            kernel,
            in_specs=ins,
            out_specs=spaces or [VMEM] * len(outs),
            input_output_aliases=aliases,
            out_shape=[shape(s, t) for s, t in outs],
            scratch_shapes=scratches,
            compiler_params=pltpu.CompilerParams(vmem_limit_bytes=mib * 2**20),
            cost_estimate=pl.CostEstimate(flops=flops, bytes_accessed=8_000_000, transcendentals=0),
        )

    def swap(value, axis, odd):
        count = lax.axis_size(axis)
        pairs = [(i, i + 1) for i in range(1 if odd else 0, count - 1, 2)]
        return lax.ppermute(value, axis, pairs + [(j, i) for i, j in pairs])

    tip, mid = ((2 * HALO, LANES), f32), ((rows - 2 * HALO, LANES), f32)
    edge, corner = ((HALO, width), f32), ((HALO, 2 * LANES), f32)
    sends = call(pack_kernel, [HBM], [tip, tip, mid, mid, edge, edge], [pltpu.SemaphoreType.DMA((8,))], 52, 1000)(x)
    b_ends = swap(sends[1], "cols", True)
    a_ends = swap(sends[0], "cols", False)
    b_mid = swap(sends[3], "cols", True)
    a_mid = swap(sends[2], "cols", False)
    by_y = swap(sends[4], "rows", True)
    by_core = swap(sends[5], "rows", False)
    to_y, to_core = call(corner_kernel, [VMEM, VMEM], [corner, corner], [], 2, 1000)(a_ends, b_ends)
    corner_y = swap(to_y, "rows", True)
    corner_core = swap(to_core, "rows", False)

    few = 2 * BORDER
    at_left, at_right = tents(width, True, False), tents(width, False, True)
    at_left = jnp.concatenate([at_left[:few], at_left[width + LANES - few :]], axis=0)
    at_right = at_right[width - few : width + few]
    level_rows = (tall + BORDER, rows // 2 + 3 * BORDER, rows // 4 + 2 * BORDER, rows // 8)
    early = call(
        early_kernel,
        [VMEM] * 3,
        [
            ((3, most, LANES), f32),
            ((3, most, LANES), f32),
            ((tiles, deep + 8, LANES), f32),
            ((most, LANES), f32),
            *(((tiles - 2, n, LANES), f32) for n in level_rows),
        ],
        [
            scratch(deep + 8, LANES),
            scratch(deep + 8, LANES),
            scratch(tiles, most, LANES),
            scratch(tiles, most, LANES),
            *[scratch(SLOTS, width + 2 * HALO + 8, LANES)] * 4,
            scratch(2 * (tiles - 2), most + 2 * BORDER, LANES),
            pltpu.SemaphoreType.DMA((tiles,)),
        ],
        20,
        80_000_000,
    )(x, by_core, by_y)
    strip, pairs = ((2, deep + 8, LANES), f32), ((4, deep + 8, LANES), f32)
    scanning = [scratch(4 * TURNS, LANES + 16, LANES), scratch(4 * TURNS, LANES + 8, LANES), *[scratch(deep + 8, LANES)] * 2]
    wall = ((4, tall, LANES), f32)
    *early, u1, u2, u3 = early
    parts = [
        ((width + LANES, width // 2 + width // 4 + LANES), bf16),
        ((rows // 2, width // 2), f32),
        ((rows // 4, width // 4), f32),
        ((rows // 8, LANES), f32),
    ]
    middle = call(middle_kernel, [VMEM] * 11, [strip, pairs, wall, *parts], scanning, 8, 10_000_000)(
        a_ends, b_ends, corner_core, corner_y, b_mid, u1, u2, u3, tents(width, False, False), at_left, at_right
    )
    *outs, third = call(
        late_kernel,
        [VMEM] * 13,
        [strip, pairs, wall] + [((rows >> k, width >> k), f32) for k in range(3)] + [((width // 8, rows // 8), f32)],
        scanning
        + [
            scratch(6, tall + 3 * BORDER, LANES),
            *(scratch(3, n, LANES) for n in level_rows),
            scratch(rows // 2, width // 2),
            scratch(rows // 4, width // 4),
            scratch(width // 8, rows // 8),
            pltpu.SemaphoreType.DMA((tiles + 3,)),
        ],
        20,
        80_000_000,
        [VMEM] * 3 + [ANY] * 4,
        {1: 0, 2: 1, 3: 2},
    )(a_mid, *middle, *early)
    return (*outs[3:], third.T)


def solution(mesh):
    spec = P("rows", "cols")

    return jax.shard_map(on_device, mesh=mesh, in_specs=(spec,), out_specs=(spec,) * 4, check_vma=False)
```
